32 devices in a mesh: space: 8 (over y, x, core), level: 4 (over z).
Axes of the slice: x: 2, y: 2, z: 4, core: 2. Of those that a mesh axis runs over, the one named last changes fastest.
Arguments:
- levels_in: bfloat16 [12, 48, 384, 512], P('level', 'space'), may hold values from -6 to 6
- kv_gain: float32 [512], replicated, may hold values from 0.25 to 1.75
- level_embed: float32 [12, 512], P('level'), may hold values from -3 to 3
- latent_queries: float32 [3, 512], replicated, may hold values from -6 to 6
- q_weight: bfloat16 [512, 512], replicated, may hold values from -0.25 to 0.25
- k_weight: bfloat16 [512, 512], replicated, may hold values from -0.25 to 0.25
- v_weight: bfloat16 [512, 512], replicated, may hold values from -0.25 to 0.25
- out_weight: bfloat16 [512, 512], replicated, may hold values from -0.25 to 0.25
- perc_scale: float32 [8], replicated, may hold values from 4 to 24
- attn_gain: float32 [512], replicated, may hold values from 0.25 to 1.75
- qkv_weight: bfloat16 [512, 1536], replicated, may hold values from -0.25 to 0.25
- swin_scale: float32 [8], replicated, may hold values from 4 to 24
- proj_weight: bfloat16 [512, 512], replicated, may hold values from -0.25 to 0.25
- mlp_gain: float32 [512], replicated, may hold values from 0.25 to 1.75
- up_weight: bfloat16 [512, 2048], replicated, may hold values from -0.25 to 0.25
- down_weight: bfloat16 [2048, 512], replicated, may hold values from -0.125 to 0.125
Outputs:
- latent_out: bfloat16 [3, 48, 384, 512], P(None, 'space', 'level')
The draws below stay inside these ranges and needn't reach their ends.
All inputs are finite; a program needn't handle non-finite values.
Results may differ from the reference program's by a relative error of at most 0.017.
Values may be sent and summed in bfloat16 or wider, within the bound.
A program may use at most 128 MiB of HBM per device.

```python
import math
import jax
import jax.numpy as jnp
from jax import lax

D = 512
HEADS = 8
MLP = 2048
LEVELS = 12
LATENT = 3
WR = 6
WC = 12
HEAD_DIM = 64
SR = 3
SC = 6
ROWS = 48
COLS = 384


def steps_of(key, dims, cuts, low, high):
    factor_of = 1.0
    for dim, blocks in cuts:
        steps = jax.random.uniform(jax.random.fold_in(jax.random.fold_in(key, 6), dim), (blocks,), jnp.float32, low / len(cuts), high / len(cuts))
        factor_of = factor_of * jnp.repeat(jnp.exp(steps), dims[dim] // blocks).reshape((-1,) + (1,) * (len(dims) - 1 - dim))
    return factor_of


def bell_draw(rng, dims, scale, bound, cuts=(), kind=jnp.bfloat16):
    values = jax.random.normal(rng, dims, jnp.float32) * scale
    if len(cuts) > 0:
        values = steps_of(rng, dims, cuts, -0.22, 0.18) * values
    return jnp.clip(values, min=-bound, max=bound).astype(kind)


def setup_inputs(seed: int = 0) -> dict:
    key_list = jax.random.split(jax.random.key(seed), 17)
    return {
        "levels_in": bell_draw(key_list[0], (LEVELS, ROWS, COLS, D), 1.0, 6.0, ((0, 4), (1, 8))),
        "kv_gain": jnp.clip(1.0 + 0.15 * jax.random.normal(key_list[1], (D,), jnp.float32), 0.25, 1.75),
        "level_embed": bell_draw(key_list[2], (LEVELS, D), 0.5, 3.0, ((0, 4),), jnp.float32),
        "latent_queries": bell_draw(key_list[3], (LATENT, D), 1.0, 6.0, (), jnp.float32),
        "q_weight": bell_draw(key_list[4], (D, D), D ** -0.5, 0.25),
        "k_weight": bell_draw(key_list[5], (D, D), D ** -0.5, 0.25),
        "v_weight": bell_draw(key_list[6], (D, D), D ** -0.5, 0.25),
        "out_weight": bell_draw(key_list[7], (D, D), D ** -0.5, 0.25),
        "perc_scale": jnp.clip(jnp.exp(jax.random.uniform(key_list[8], (HEADS,), jnp.float32, math.log(4.0), math.log(24.0))), 4.0, 24.0),
        "attn_gain": jnp.clip(1.0 + 0.15 * jax.random.normal(key_list[9], (D,), jnp.float32), 0.25, 1.75),
        "qkv_weight": bell_draw(key_list[10], (D, 3 * D), D ** -0.5, 0.25),
        "swin_scale": jnp.clip(jnp.exp(jax.random.uniform(key_list[11], (HEADS,), jnp.float32, math.log(4.0), math.log(24.0))), 4.0, 24.0),
        "proj_weight": bell_draw(key_list[12], (D, D), D ** -0.5, 0.25),
        "mlp_gain": jnp.clip(1.0 + 0.15 * jax.random.normal(key_list[13], (D,), jnp.float32), 0.25, 1.75),
        "up_weight": bell_draw(key_list[14], (D, MLP), D ** -0.5, 0.25),
        "down_weight": bell_draw(key_list[15], (MLP, D), MLP ** -0.5, 0.125),
    }


def layer_norm(values, gain):
    center = values - lax.optimization_barrier(jnp.mean(values, -1, keepdims=True))
    spread = lax.optimization_barrier(jnp.mean(center * center, -1, keepdims=True))
    return center * lax.rsqrt(spread + 1e-05) * gain

def unit_heads(values):
    return values * lax.rsqrt(lax.optimization_barrier(jnp.mean(values * values, -1, keepdims=True)) + 1e-06)

def perceiver_pool(tokens, query_unit, k_weight, v_weight, perc_scale):
    levels, rows, cols, width = tokens.shape
    heads = query_unit.shape[1]
    head_dim = width // heads
    keys = jnp.dot(tokens, k_weight, preferred_element_type=jnp.float32).astype(jnp.bfloat16)
    values = jnp.dot(tokens, v_weight, preferred_element_type=jnp.float32).astype(jnp.bfloat16)
    key_unit = unit_heads(keys.astype(jnp.float32).reshape(levels, rows, cols, heads, head_dim))
    scores = jnp.einsum('ahd,lrchd->alrch', query_unit, key_unit, precision=lax.Precision.HIGHEST)
    scores = scores * (perc_scale / head_dim)
    weights = jnp.exp(scores)
    denom = lax.optimization_barrier(jnp.sum(weights, axis=1))
    split_values = values.reshape(levels, rows, cols, heads, head_dim).astype(jnp.float32)
    weights_low = weights.astype(jnp.bfloat16).astype(jnp.float32)
    numer = jnp.einsum('alrch,lrchd->archd', weights_low, split_values, precision=lax.Precision.HIGHEST)
    pooled = numer / denom[..., None]
    return pooled.reshape(pooled.shape[0], rows, cols, width).astype(jnp.bfloat16)

def swin_block(block, first_row, total_rows, attn_gain, qkv_weight, swin_scale, proj_weight, mlp_gain, up_weight, down_weight):
    latent_count, rows, cols, width = block.shape
    heads = swin_scale.shape[0]
    head_dim = width // heads
    window_count = cols // WC
    tokens_per = latent_count * rows * WC
    normed = layer_norm(block.astype(jnp.float32), attn_gain).astype(jnp.bfloat16)
    packed = jnp.dot(normed, qkv_weight, preferred_element_type=jnp.float32).astype(jnp.bfloat16)
    windows = packed.reshape(latent_count, rows, window_count, WC, 3 * width).transpose(2, 0, 1, 3, 4)
    windows = windows.reshape(window_count, tokens_per, 3, heads, head_dim)
    query_part = unit_heads(windows[:, :, 0].astype(jnp.float32))
    key_part = unit_heads(windows[:, :, 1].astype(jnp.float32))
    value_part = windows[:, :, 2].astype(jnp.float32)
    scores = jnp.einsum('wihd,wjhd->whij', query_part, key_part, precision=lax.Precision.HIGHEST)
    scores = scores * (swin_scale / head_dim)[:, None, None]
    position = jnp.arange(tokens_per, dtype=jnp.int32) // WC % rows + first_row
    region = (position >= total_rows - WR).astype(jnp.int32) + (position >= total_rows - SR).astype(jnp.int32)
    allowed = region[:, None] == region[None, :]
    weights = jnp.where(allowed, jnp.exp(scores), jnp.float32(0.0))
    probs = (weights / lax.optimization_barrier(jnp.sum(weights, -1, keepdims=True))).astype(jnp.bfloat16)
    mixed = jnp.einsum('whij,wjhd->wihd', probs.astype(jnp.float32), value_part, precision=lax.Precision.HIGHEST)
    mixed = mixed.astype(jnp.bfloat16).reshape(window_count, latent_count, rows, WC, width)
    mixed = mixed.transpose(1, 2, 0, 3, 4).reshape(latent_count, rows, cols, width)
    branch = jnp.dot(mixed, proj_weight, preferred_element_type=jnp.float32).astype(jnp.bfloat16)
    middle = block.astype(jnp.float32) + branch.astype(jnp.float32)
    mlp_in = layer_norm(middle, mlp_gain).astype(jnp.bfloat16)
    hidden = jax.nn.gelu(jnp.dot(mlp_in, up_weight, preferred_element_type=jnp.float32)).astype(jnp.bfloat16)
    final = middle + jnp.dot(hidden, down_weight, preferred_element_type=jnp.float32)
    return final.astype(jnp.bfloat16)

def reference(levels_in, kv_gain, level_embed, latent_queries, q_weight, k_weight, v_weight, out_weight, perc_scale, attn_gain, qkv_weight, swin_scale, proj_weight, mlp_gain, up_weight, down_weight):
    queries = jnp.dot(latent_queries.astype(jnp.bfloat16), q_weight, preferred_element_type=jnp.float32)
    query_unit = unit_heads(queries.reshape(LATENT, HEADS, HEAD_DIM))
    block_count = ROWS // WR

    def encode(index):
        start = (index * WR).astype(jnp.int32)
        raw = lax.dynamic_slice_in_dim(levels_in, start, WR, 1)
        tokens = (layer_norm(raw.astype(jnp.float32), kv_gain) + level_embed[:, None, None, :]).astype(jnp.bfloat16)
        pooled = perceiver_pool(tokens, query_unit, k_weight, v_weight, perc_scale)
        latent = latent_queries[:, None, None, :] + jnp.dot(pooled, out_weight, preferred_element_type=jnp.float32)
        return latent.astype(jnp.bfloat16)
    blocks = lax.map(encode, jnp.arange(block_count, dtype=jnp.int32))
    latent = blocks.transpose(1, 0, 2, 3, 4).reshape(LATENT, ROWS, COLS, D)
    rolled = jnp.roll(latent, (-SR, -SC), axis=(1, 2))

    def layer(index):
        start = (index * WR).astype(jnp.int32)
        block = lax.dynamic_slice_in_dim(rolled, start, WR, 1)
        return swin_block(block, start, ROWS, attn_gain, qkv_weight, swin_scale, proj_weight, mlp_gain, up_weight, down_weight)
    finals = lax.map(layer, jnp.arange(block_count, dtype=jnp.int32))
    final = finals.transpose(1, 0, 2, 3, 4).reshape(LATENT, ROWS, COLS, D)
    return jnp.roll(final, (SR, SC), axis=(1, 2))
```

```python
import functools

import jax
import jax.numpy as jnp
from jax import lax
from jax.experimental import pallas as pl
from jax.experimental.pallas import tpu as pltpu
from jax.sharding import PartitionSpec as P

WR = 6
WC = 12
SR = 3
SC = 6
LANES = 128
STEP = 2 * WC
EDGE = 8
BF = jnp.bfloat16
F32 = jnp.float32
MESH = pl.DeviceIdType.MESH


def dot(a, b):
    return jnp.dot(a, b, preferred_element_type=F32)


def dot_t(a, b):
    return lax.dot_general(a, b, (((1,), (1,)), ((), ())), preferred_element_type=F32)


def iota(shape, axis):
    return lax.broadcasted_iota(jnp.int32, shape, axis)


def layer_norm(values, gain):
    center = values - jnp.mean(values, -1, keepdims=True)
    spread = jnp.mean(center * center, -1, keepdims=True)
    return center * lax.rsqrt(spread + 1e-05) * gain


def kernel(
    levels_hbm,
    kv_gain,
    embed,
    lq,
    q_hbm,
    k_hbm,
    v_hbm,
    out_hbm,
    perc,
    attn_gain,
    qkv_hbm,
    swin,
    proj_hbm,
    mlp_gain,
    up_hbm,
    down_hbm,
    p_hbm,
    q_w,
    k_w,
    v_w,
    out_w,
    qkv_w,
    proj_w,
    up_w,
    down_w,
    xa,
    xb,
    mine,
    from_left,
    from_right,
    total,
    head,
    tail,
    ahead,
    own,
    back,
    q_mat,
    ones,
    spread,
    den_spread,
    ones_t,
    padded,
    w_sem,
    xa_sem,
    xb_sem,
    z_send,
    left_recv,
    right_recv,
    head_send,
    head_recv,
    own_sem,
    back_send,
    back_recv,
    edge_send,
    edge_recv,
):
    levels, rows, all_cols, width = levels_hbm.shape
    latents = lq.shape[0]
    heads = perc.shape[0]
    head_dim = width // heads
    n = lax.axis_size("level")
    spaces = lax.axis_size("space")
    me = lax.axis_index("level")
    place = lax.axis_index("space")
    cols = all_cols // n
    chunks = cols // STEP
    tokens = rows * STEP
    half = SR * STEP
    side = latents * half
    packed_rows = latents * tokens + 16

    up_level = lax.rem(me + 1, n)
    down_level = lax.rem(me + n - 1, n)
    up_space = lax.rem(place + 1, spaces)
    down_space = lax.rem(place + spaces - 1, spaces)

    barrier = pltpu.get_barrier_semaphore()
    for target in (
        {"level": up_level},
        {"level": down_level},
        {"space": up_space},
        {"space": down_space},
        {"space": up_space, "level": up_level},
        {"space": down_space, "level": down_level},
    ):
        pl.semaphore_signal(barrier, inc=1, device_id=target, device_id_type=MESH)

    def dest_of(j):
        return jnp.where(2 * me < n, n - 1 - j, j)

    def chunk_of(i):
        return lax.rem(i + chunks - 1, chunks)

    def weight_copies():
        pairs = (
            (q_hbm, q_w),
            (k_hbm, k_w),
            (v_hbm, v_w),
            (out_hbm, out_w),
            (qkv_hbm, qkv_w),
            (proj_hbm, proj_w),
            (up_hbm, up_w),
            (down_hbm, down_w),
        )
        return [pltpu.make_async_copy(a, b, w_sem.at[i]) for i, (a, b) in enumerate(pairs)]

    def x_copies(i, j):
        slot = lax.rem(i, 2) * n + j
        start = pl.multiple_of(dest_of(j) * cols + chunk_of(i) * STEP, EDGE)
        rest = pl.multiple_of(lax.rem(start + STEP, all_cols), EDGE)
        return (
            pltpu.make_async_copy(
                levels_hbm.at[:, :, pl.ds(start, STEP)], xa.at[slot], xa_sem.at[slot]
            ),
            pltpu.make_async_copy(
                levels_hbm.at[:, :, pl.ds(rest, EDGE)], xb.at[slot], xb_sem.at[slot]
            ),
        )

    def start_x(i):
        def body(j, carry):
            for copy in x_copies(i, j):
                copy.start()
            return carry

        lax.fori_loop(0, n, body, 0)

    def send_right(d, i):
        return pltpu.make_async_remote_copy(
            src_ref=mine.at[d, i],
            dst_ref=from_left.at[d, i],
            send_sem=z_send.at[d, i],
            recv_sem=left_recv.at[d, i],
            device_id={"level": up_level},
            device_id_type=MESH,
        )

    def send_left(d, i):
        return pltpu.make_async_remote_copy(
            src_ref=mine.at[d, i],
            dst_ref=from_right.at[d, i],
            send_sem=z_send.at[d, i],
            recv_sem=right_recv.at[d, i],
            device_id={"level": down_level},
            device_id_type=MESH,
        )

    def send_head(i):
        return pltpu.make_async_remote_copy(
            src_ref=head.at[i],
            dst_ref=ahead.at[i],
            send_sem=head_send.at[i],
            recv_sem=head_recv.at[i],
            device_id={"space": down_space},
            device_id_type=MESH,
        )

    def column_of(i):
        return pl.multiple_of(EDGE + chunk_of(i) * STEP, EDGE)

    def send_back(i):
        return pltpu.make_async_remote_copy(
            src_ref=back.at[i],
            dst_ref=p_hbm.at[:, pl.ds(0, SR), pl.ds(column_of(i), STEP)],
            send_sem=back_send.at[i],
            recv_sem=back_recv.at[i],
            device_id={"space": up_space},
            device_id_type=MESH,
        )

    def keep_own(i):
        return pltpu.make_async_copy(
            own.at[i],
            p_hbm.at[:, pl.ds(SR, SR), pl.ds(column_of(i), STEP)],
            own_sem.at[i],
        )

    def edge_copies():
        cut = pl.ds(STEP - EDGE, EDGE)
        return (
            pltpu.make_async_remote_copy(
                src_ref=own.at[0, :, :, cut],
                dst_ref=p_hbm.at[:, pl.ds(SR, SR), pl.ds(0, EDGE)],
                send_sem=edge_send.at[0],
                recv_sem=edge_recv.at[0],
                device_id={"level": up_level},
                device_id_type=MESH,
            ),
            pltpu.make_async_remote_copy(
                src_ref=back.at[0, :, :, cut],
                dst_ref=p_hbm.at[:, pl.ds(0, SR), pl.ds(0, EDGE)],
                send_sem=edge_send.at[1],
                recv_sem=edge_recv.at[1],
                device_id={"space": up_space, "level": up_level},
                device_id_type=MESH,
            ),
        )

    weights = weight_copies()
    weights[0].start()
    weights[1].start()
    weights[2].start()
    start_x(0)

    lane = iota((latents, width), 1) // head_dim
    ones[...] = (
        (iota((width, LANES), 0) // head_dim == lax.rem(iota((width, LANES), 1), heads))
        & (iota((width, LANES), 1) < latents * heads)
    ).astype(F32).astype(BF)
    for a in range(latents):
        spread[:, a * width : (a + 1) * width] = (
            iota((LANES, width), 0) == iota((LANES, width), 1) // head_dim + a * heads
        ).astype(F32).astype(BF)
    for t in range(2):
        den_spread[t] = (
            iota((16, width), 0) - t * heads == iota((16, width), 1) // head_dim
        ).astype(F32).astype(BF)
    ones_t[...] = (iota((16, width), 0) == iota((16, width), 1) // head_dim).astype(F32).astype(BF)

    padded[...] = jnp.zeros_like(padded)
    padded[0:latents, :] = lq[...]
    weights[0].wait()
    queries = dot(padded[...].astype(BF), q_w[...])[:8]
    squares = queries * queries
    lane8 = iota((8, width), 1) // head_dim
    factor = jnp.zeros((8, width), F32)
    for h in range(heads):
        mean = jnp.sum(jnp.where(lane8 == h, squares, 0.0), -1, keepdims=True) / head_dim
        scale = lax.rsqrt(mean + 1e-06) * (perc[h] / head_dim)
        factor = jnp.where(lane8 == h, scale, factor)
    unit = queries * factor
    own_head = iota((heads, width), 0) == iota((heads, width), 1) // head_dim
    parts = [jnp.where(own_head, unit[a : a + 1], 0.0) for a in range(latents)]
    parts.append(jnp.zeros((LANES - latents * heads, width), F32))
    q_rows = jnp.concatenate(parts, 0)
    q_high = q_rows.astype(BF)
    q_mat[:LANES, :] = q_high
    q_mat[LANES:, :] = (q_rows - q_high.astype(F32)).astype(BF)

    weights[1].wait()
    weights[2].wait()
    for copy in weights[3:]:
        copy.start()
    pl.semaphore_wait(barrier, 6)

    def partial(i, j):
        slot = lax.rem(i, 2) * n + j
        d = dest_of(j)
        for copy in x_copies(i, j):
            copy.wait()
        normed = []
        for l in range(levels):
            x = jnp.concatenate([xa[slot, l].astype(F32), xb[slot, l].astype(F32)], 1)
            x = x[:, SC : SC + STEP].reshape(tokens, width)
            x = layer_norm(x, kv_gain[...]) + embed[l : l + 1, :]
            normed.append(x.astype(BF))
        normed = jnp.concatenate(normed, 0)
        keys = dot(normed, k_w[...]).astype(BF)
        values = dot(normed, v_w[...]).astype(BF).astype(F32)
        keys32 = keys.astype(F32)
        squares = dot((keys32 * keys32).astype(BF), ones[...])
        raw = dot_t(keys, q_mat[...])
        raw = raw[:, :LANES] + raw[:, LANES:]
        weights = jnp.exp(raw * lax.rsqrt(squares * (1.0 / head_dim) + 1e-06))
        denom = weights[:tokens]
        for l in range(1, levels):
            denom = denom + weights[l * tokens : (l + 1) * tokens]
        low = weights.astype(BF)
        for a in range(latents):
            wide = dot(low, spread[:, a * width : (a + 1) * width]) * values
            numer = wide[:tokens]
            for l in range(1, levels):
                numer = numer + wide[l * tokens : (l + 1) * tokens]
            mine[d, i, a * tokens : (a + 1) * tokens, :] = numer.astype(BF)
        pad = 2 * LANES - tokens
        turned = jnp.concatenate([denom, jnp.ones((pad, LANES), F32)], 0).T
        halves = []
        for t in range(2):
            cut = slice(t * LANES, (t + 1) * LANES)
            row = [turned[a * 8 : a * 8 + 8, cut] for a in range(latents)]
            row.append(jnp.ones((8, width - latents * LANES), F32))
            halves.append(jnp.concatenate(row, 1))
        mine[d, i, latents * tokens :, :] = jnp.concatenate(halves, 0).astype(BF)

        @pl.when((me == 0) & (d != me))
        def _():
            send_right(d, i).start()

        @pl.when((me == n - 1) & (d != me))
        def _():
            send_left(d, i).start()

    def forward(i, j):
        d = dest_of(j)

        @pl.when((d > me) & (me > 0))
        def _():
            send_right(d, i).wait_recv()
            mine[d, i] = (mine[d, i].astype(F32) + from_left[d, i].astype(F32)).astype(BF)
            send_right(d, i).start()

        @pl.when((d < me) & (me < n - 1))
        def _():
            send_left(d, i).wait_recv()
            mine[d, i] = (mine[d, i].astype(F32) + from_right[d, i].astype(F32)).astype(BF)
            send_left(d, i).start()

    def latent(i):
        total[...] = mine[me, i].astype(F32)

        @pl.when(me > 0)
        def _():
            send_right(me, i).wait_recv()
            total[...] += from_left[me, i].astype(F32)

        @pl.when(me < n - 1)
        def _():
            send_left(me, i).wait_recv()
            total[...] += from_right[me, i].astype(F32)

        turned = total[latents * tokens :, :].T.astype(BF)
        for a in range(latents):
            block = turned[a * LANES : (a + 1) * LANES]
            denom = jnp.concatenate(
                [dot(block, den_spread[0]), dot(block, den_spread[1])[: tokens - LANES]], 0
            )
            pooled = (total[a * tokens : (a + 1) * tokens, :] / denom).astype(BF)
            value = lq[a : a + 1, :] + dot(pooled, out_w[...])
            head[i, a] = value[:half].astype(BF)
            tail[a] = value[half:].astype(BF)
        send_head(i).start()

    scale_row = jnp.zeros((1, LANES), F32)
    for h in range(heads):
        scale_row = jnp.where(iota((1, LANES), 1) == h, swin[h] / head_dim, scale_row)

    def layer(i):
        send_head(i).wait_recv()
        block = jnp.concatenate(
            [
                tail[...].astype(F32).reshape(side, width),
                ahead[i].astype(F32).reshape(side, width),
            ],
            0,
        )
        normed = layer_norm(block, attn_gain[...]).astype(BF)
        packed = dot(normed, qkv_w[...]).astype(BF)
        q = packed[:, :width]
        k = packed[:, width : 2 * width]
        v = packed[:, 2 * width :]
        q32 = q.astype(F32)
        k32 = k.astype(F32)
        q_norm = dot((q32 * q32).astype(BF), ones[...])
        q_norm = lax.rsqrt(q_norm * (1.0 / head_dim) + 1e-06) * scale_row
        k_norm = dot_t(ones_t[...], (k32 * k32).astype(BF))
        k_norm = lax.rsqrt(k_norm * (1.0 / head_dim) + 1e-06)
        row = iota((2 * side, 2 * side), 0)
        col = iota((2 * side, 2 * side), 1)
        window = lax.rem(row, STEP) // WC == lax.rem(col, STEP) // WC
        region = (row >= side) == (col >= side)
        mask = jnp.where(window & (region | (place < spaces - 1)), 1.0, 0.0)
        mixed = []
        for h in range(heads):
            cut = slice(h * head_dim, (h + 1) * head_dim)
            scores = dot_t(q[:, cut], k[:, cut])
            scores = scores * q_norm[:, h : h + 1] * k_norm[h : h + 1, :]
            weights = jnp.exp(scores) * mask
            norm = jnp.sum(weights, -1, keepdims=True)
            mixed.append(dot(weights.astype(BF), v[:, cut]) / norm)
        mixed = jnp.concatenate(mixed, 1).astype(BF)
        branch = dot(mixed, proj_w[...]).astype(BF)
        middle = block + branch.astype(F32)
        mlp_in = layer_norm(middle, mlp_gain[...]).astype(BF)
        hidden = jax.nn.gelu(dot(mlp_in, up_w[...])).astype(BF)
        final = middle + dot(hidden, down_w[...])
        own[i] = final[:side].reshape(latents, SR, STEP, width).astype(BF)
        back[i] = final[side:].reshape(latents, SR, STEP, width).astype(BF)
        keep_own(i).start()
        send_back(i).start()

        @pl.when(i == 0)
        def _():
            for copy in edge_copies():
                copy.start()

    def step(s, carry):
        t = s - 1

        @pl.when(t >= 1)
        def _():
            @pl.when(t == 1)
            def _():
                for copy in weights[3:]:
                    copy.wait()

            latent(t - 1)

        @pl.when(t + 2 < chunks)
        def _():
            start_x(t + 2)

        @pl.when(t + 1 < chunks)
        def _():
            def body(j, c):
                partial(t + 1, j)
                return c

            lax.fori_loop(0, n, body, 0)

        @pl.when(t >= 1)
        def _():
            layer(t - 1)

        @pl.when((t >= 0) & (t < chunks))
        def _():
            def body(j, c):
                forward(t, j)
                return c

            lax.fori_loop(0, n, body, 0)

        return carry

    lax.fori_loop(0, chunks + 2, step, 0)

    def drain(i, carry):
        def each(d, c):
            @pl.when(d != me)
            def _():
                send_right(d, i).wait_send()

            return c

        lax.fori_loop(0, n, each, 0)
        send_head(i).wait_send()
        keep_own(i).wait()
        send_back(i).wait()
        return carry

    lax.fori_loop(0, chunks, drain, 0)
    for copy in edge_copies():
        copy.wait()


def shards(
    levels_in,
    kv_gain,
    level_embed,
    latent_queries,
    q_weight,
    k_weight,
    v_weight,
    out_weight,
    perc_scale,
    attn_gain,
    qkv_weight,
    swin_scale,
    proj_weight,
    mlp_gain,
    up_weight,
    down_weight,
):
    levels, rows, all_cols, width = levels_in.shape
    latents = latent_queries.shape[0]
    heads = perc_scale.shape[0]
    mlp = up_weight.shape[1]
    n = lax.axis_size("level")
    cols = all_cols // n
    chunks = cols // STEP
    tokens = rows * STEP
    half = SR * STEP
    packed_rows = latents * tokens + 16
    assert rows == WR and heads == 8 and LANES < tokens <= 2 * LANES
    assert cols % STEP == 0 and n >= 2

    hbm = pl.BlockSpec(memory_space=pl.ANY)
    vmem = pl.BlockSpec(memory_space=pltpu.VMEM)
    smem = pl.BlockSpec(memory_space=pltpu.SMEM)
    sem = pltpu.SemaphoreType.DMA
    padded = pl.pallas_call(
        kernel,
        in_specs=[hbm, vmem, vmem, vmem, hbm, hbm, hbm, hbm, smem, vmem, hbm, smem, hbm, vmem]
        + [hbm, hbm],
        out_specs=hbm,
        out_shape=jax.ShapeDtypeStruct((latents, rows, cols + EDGE, width), BF),
        scratch_shapes=[
            pltpu.VMEM((width, width), BF),
            pltpu.VMEM((width, width), BF),
            pltpu.VMEM((width, width), BF),
            pltpu.VMEM((width, width), BF),
            pltpu.VMEM((width, 3 * width), BF),
            pltpu.VMEM((width, width), BF),
            pltpu.VMEM((width, mlp), BF),
            pltpu.VMEM((mlp, width), BF),
            pltpu.VMEM((2 * n, levels, rows, STEP, width), BF),
            pltpu.VMEM((2 * n, levels, rows, EDGE, width), BF),
            pltpu.VMEM((n, chunks, packed_rows, width), BF),
            pltpu.VMEM((n, chunks, packed_rows, width), BF),
            pltpu.VMEM((n, chunks, packed_rows, width), BF),
            pltpu.VMEM((packed_rows, width), F32),
            pltpu.VMEM((chunks, latents, half, width), BF),
            pltpu.VMEM((latents, half, width), BF),
            pltpu.VMEM((chunks, latents, half, width), BF),
            pltpu.VMEM((chunks, latents, SR, STEP, width), BF),
            pltpu.VMEM((chunks, latents, SR, STEP, width), BF),
            pltpu.VMEM((2 * LANES, width), BF),
            pltpu.VMEM((width, LANES), BF),
            pltpu.VMEM((LANES, latents * width), BF),
            pltpu.VMEM((2, 16, width), BF),
            pltpu.VMEM((16, width), BF),
            pltpu.VMEM((16, width), F32),
            sem((8,)),
            sem((2 * n,)),
            sem((2 * n,)),
            sem((n, chunks)),
            sem((n, chunks)),
            sem((n, chunks)),
            sem((chunks,)),
            sem((chunks,)),
            sem((chunks,)),
            sem((chunks,)),
            sem((chunks,)),
            sem((2,)),
            sem((2,)),
        ],
        compiler_params=pltpu.CompilerParams(
            collective_id=0, has_side_effects=True, vmem_limit_bytes=63 * 1024 * 1024
        ),
        name="whole",
    )(
        levels_in,
        kv_gain[None],
        level_embed,
        latent_queries,
        q_weight,
        k_weight,
        v_weight,
        out_weight,
        perc_scale,
        attn_gain[None],
        qkv_weight,
        swin_scale,
        proj_weight,
        mlp_gain[None],
        up_weight,
        down_weight,
    )
    return padded[:, :, EDGE - SC : EDGE - SC + cols]


def solution(mesh):
    placed = (P("level", "space", None, None), P(), P("level", None)) + (P(),) * 13
    return jax.shard_map(
        shards,
        mesh=mesh,
        in_specs=placed,
        out_specs=P(None, "space", "level", None),
        check_vma=False,
    )
```

```python
import functools

import jax
import jax.numpy as jnp
from jax import lax
from jax.experimental import pallas as pl
from jax.experimental.pallas import tpu as pltpu
from jax.sharding import PartitionSpec as P

WR = 6
WC = 12
SR = 3
SC = 6
LANES = 128
STEP = 2 * WC
EDGE = 8
LEAD = 2
BF = jnp.bfloat16
F32 = jnp.float32
MESH = pl.DeviceIdType.MESH


def dot(a, b):
    return jnp.dot(a, b, preferred_element_type=F32)


def dot_t(a, b):
    return lax.dot_general(a, b, (((1,), (1,)), ((), ())), preferred_element_type=F32)


def iota(shape, axis):
    return lax.broadcasted_iota(jnp.int32, shape, axis)


def layer_norm(values, gain):
    center = values - jnp.mean(values, -1, keepdims=True)
    spread = jnp.mean(center * center, -1, keepdims=True)
    return center * lax.rsqrt(spread + 1e-05) * gain


def kernel(
    levels_hbm,
    kv_gain,
    embed,
    lq,
    q_hbm,
    k_hbm,
    v_hbm,
    out_hbm,
    perc,
    attn_gain,
    qkv_hbm,
    swin,
    proj_hbm,
    mlp_gain,
    up_hbm,
    down_hbm,
    p_hbm,
    q_w,
    k_w,
    v_w,
    out_w,
    qkv_w,
    proj_w,
    up_w,
    down_w,
    xa,
    xb,
    mine,
    arrived,
    head,
    tail,
    ahead,
    own,
    back,
    q_mat,
    ones,
    spread,
    den_spread,
    ones_t,
    padded,
    mask,
    w_sem,
    xa_sem,
    xb_sem,
    z_send,
    z_recv,
    head_send,
    head_recv,
    own_sem,
    back_send,
    back_recv,
    edge_send,
    edge_recv,
):
    levels, rows, all_cols, width = levels_hbm.shape
    latents = lq.shape[0]
    heads = perc.shape[0]
    head_dim = width // heads
    n = lax.axis_size("level")
    spaces = lax.axis_size("space")
    me = lax.axis_index("level")
    place = lax.axis_index("space")
    cols = all_cols // n
    chunks = cols // STEP
    units = 2 * chunks
    tokens = SR * STEP
    side = latents * tokens
    raw_rows = levels * tokens
    lead = LEAD
    is_end = (me == 0) | (me == n - 1)

    up_level = lax.rem(me + 1, n)
    down_level = lax.rem(me + n - 1, n)
    up_space = lax.rem(place + 1, spaces)
    down_space = lax.rem(place + spaces - 1, spaces)

    barrier = pltpu.get_barrier_semaphore()
    for target in (
        {"level": up_level},
        {"level": down_level},
        {"space": up_space},
        {"space": down_space},
        {"space": up_space, "level": up_level},
        {"space": down_space, "level": down_level},
    ):
        pl.semaphore_signal(barrier, inc=1, device_id=target, device_id_type=MESH)

    def dest_of(j):
        return jnp.where(2 * me < n, n - 1 - j, j)

    def lead_of(d):
        near = is_end & (jnp.abs(d - me) == 1)
        return jnp.where((d == me) | near, 0, jnp.where(d == dest_of(0), lead, lead - 1))

    def chunk_of(i):
        return lax.rem(i + chunks - 1, chunks)

    def weight_copies():
        pairs = (
            (q_hbm, q_w),
            (k_hbm, k_w),
            (v_hbm, v_w),
            (out_hbm, out_w),
            (qkv_hbm, qkv_w),
            (proj_hbm, proj_w),
            (up_hbm, up_w),
            (down_hbm, down_w),
        )
        return [pltpu.make_async_copy(a, b, w_sem.at[i]) for i, (a, b) in enumerate(pairs)]

    def x_copies(d, u):
        band = pl.ds(lax.rem(u, 2) * SR, SR)
        start = pl.multiple_of(d * cols + chunk_of(lax.div(u, 2)) * STEP, EDGE)
        rest = pl.multiple_of(lax.rem(start + STEP, all_cols), EDGE)
        return (
            pltpu.make_async_copy(
                levels_hbm.at[:, band, pl.ds(start, STEP)], xa.at[d, u], xa_sem.at[d, u]
            ),
            pltpu.make_async_copy(
                levels_hbm.at[:, band, pl.ds(rest, EDGE)], xb.at[d, u], xb_sem.at[d, u]
            ),
        )

    def each_unit(first, last, act):
        def body(k, carry):
            d = dest_of(lax.rem(k, n))
            u = lax.div(k, n) - lead + lead_of(d)

            @pl.when((u >= 0) & (u < units))
            def _():
                act(d, u)

            return carry

        lax.fori_loop(first, last, body, 0)

    def start_x(d, u):
        for copy in x_copies(d, u):
            copy.start()

    def send(d, u, right, count):
        return pltpu.make_async_remote_copy(
            src_ref=mine.at[d, u, pl.ds(0, count)],
            dst_ref=arrived.at[0 if right else 1, d, u, pl.ds(0, count)],
            send_sem=z_send.at[d, u],
            recv_sem=z_recv.at[0 if right else 1, d, u],
            device_id={"level": up_level if right else down_level},
            device_id_type=MESH,
        )

    sum_rows = mine.shape[2]

    def send_head(i):
        return pltpu.make_async_remote_copy(
            src_ref=head.at[i],
            dst_ref=ahead.at[i],
            send_sem=head_send.at[i],
            recv_sem=head_recv.at[i],
            device_id={"space": down_space},
            device_id_type=MESH,
        )

    def column_of(i):
        return pl.multiple_of(EDGE + chunk_of(i) * STEP, EDGE)

    def send_back(i):
        return pltpu.make_async_remote_copy(
            src_ref=back.at[i],
            dst_ref=p_hbm.at[:, pl.ds(0, SR), pl.ds(column_of(i), STEP)],
            send_sem=back_send.at[i],
            recv_sem=back_recv.at[i],
            device_id={"space": up_space},
            device_id_type=MESH,
        )

    def keep_own(i):
        return pltpu.make_async_copy(
            own.at[i],
            p_hbm.at[:, pl.ds(SR, SR), pl.ds(column_of(i), STEP)],
            own_sem.at[i],
        )

    def edge_copies():
        cut = pl.ds(STEP - EDGE, EDGE)
        return (
            pltpu.make_async_remote_copy(
                src_ref=own.at[0, :, :, cut],
                dst_ref=p_hbm.at[:, pl.ds(SR, SR), pl.ds(0, EDGE)],
                send_sem=edge_send.at[0],
                recv_sem=edge_recv.at[0],
                device_id={"level": up_level},
                device_id_type=MESH,
            ),
            pltpu.make_async_remote_copy(
                src_ref=back.at[0, :, :, cut],
                dst_ref=p_hbm.at[:, pl.ds(0, SR), pl.ds(0, EDGE)],
                send_sem=edge_send.at[1],
                recv_sem=edge_recv.at[1],
                device_id={"space": up_space, "level": up_level},
                device_id_type=MESH,
            ),
        )

    def level_tokens(d, u):
        for copy in x_copies(d, u):
            copy.wait()
        normed = []
        for l in range(levels):
            x = jnp.concatenate([xa[d, u, l].astype(F32), xb[d, u, l].astype(F32)], 1)
            x = x[:, SC : SC + STEP].reshape(tokens, width)
            normed.append(layer_norm(x, kv_gain[...]) + embed[l : l + 1, :])
        return jnp.concatenate(normed, 0)

    total_steps = (units + lead) * n
    early = (lead + 1) * n
    weights = weight_copies()
    each_unit(0, early, start_x)
    for copy in weights[:3]:
        copy.start()
    pl.semaphore_wait(barrier, 6)

    def send_tokens(d, u):
        @pl.when(d != me)
        def _():
            mine[d, u, :raw_rows, :] = level_tokens(d, u).astype(BF)

            @pl.when(me == 0)
            def _():
                send(d, u, True, raw_rows).start()

            @pl.when(me == n - 1)
            def _():
                send(d, u, False, raw_rows).start()

    @pl.when(is_end)
    def _():
        each_unit(0, early, send_tokens)

    each_unit(early, total_steps, start_x)
    for copy in weights[3:]:
        copy.start()

    @pl.when(is_end)
    def _():
        each_unit(early, total_steps, send_tokens)

    ones[...] = (
        (iota((width, LANES), 0) // head_dim == lax.rem(iota((width, LANES), 1), heads))
        & (iota((width, LANES), 1) < latents * heads)
    ).astype(F32).astype(BF)
    for a in range(latents):
        spread[:, a * width : (a + 1) * width] = (
            iota((LANES, width), 0) == iota((LANES, width), 1) // head_dim + a * heads
        ).astype(F32).astype(BF)
    den_spread[...] = (iota((16, width), 0) == iota((16, width), 1) // head_dim).astype(F32).astype(BF)
    ones_t[...] = den_spread[...]

    padded[...] = jnp.zeros_like(padded)
    padded[0:latents, :] = lq[...]
    weights[0].wait()
    queries = dot(padded[...].astype(BF), q_w[...])[:8]
    squares = queries * queries
    lane8 = iota((8, width), 1) // head_dim
    factor = jnp.zeros((8, width), F32)
    for h in range(heads):
        mean = jnp.sum(jnp.where(lane8 == h, squares, 0.0), -1, keepdims=True) / head_dim
        scale = lax.rsqrt(mean + 1e-06) * (perc[h] / head_dim)
        factor = jnp.where(lane8 == h, scale, factor)
    unit = queries * factor
    own_head = iota((heads, width), 0) == iota((heads, width), 1) // head_dim
    parts = [jnp.where(own_head, unit[a : a + 1], 0.0) for a in range(latents)]
    parts.append(jnp.zeros((LANES - latents * heads, width), F32))
    q_rows = jnp.concatenate(parts, 0)
    q_high = q_rows.astype(BF)
    q_mat[:LANES, :] = q_high
    q_mat[LANES:, :] = (q_rows - q_high.astype(F32)).astype(BF)

    weights[1].wait()
    weights[2].wait()

    def partial(normed):
        keys = dot(normed, k_w[...]).astype(BF)
        values = dot(normed, v_w[...]).astype(BF).astype(F32)
        keys32 = keys.astype(F32)
        squares = dot((keys32 * keys32).astype(BF), ones[...])
        raw = dot_t(keys, q_mat[...])
        raw = raw[:, :LANES] + raw[:, LANES:]
        weights = jnp.exp(raw * lax.rsqrt(squares * (1.0 / head_dim) + 1e-06))
        denom = weights[:tokens]
        count = normed.shape[0] // tokens
        for l in range(1, count):
            denom = denom + weights[l * tokens : (l + 1) * tokens]
        low = weights.astype(BF)
        parts = []
        for a in range(latents):
            wide = dot(low, spread[:, a * width : (a + 1) * width]) * values
            numer = wide[:tokens]
            for l in range(1, count):
                numer = numer + wide[l * tokens : (l + 1) * tokens]
            parts.append(numer)
        turned = jnp.concatenate([denom, jnp.ones((LANES - tokens, LANES), F32)], 0).T
        row = [turned[a * 8 : a * 8 + 8, :] for a in range(latents)]
        row.append(jnp.ones((8, width - latents * LANES), F32))
        parts.append(jnp.concatenate(row, 1))
        return jnp.concatenate(parts, 0)

    def collect(d, u):
        left = (me > 0) & (d >= me)
        right = (me < n - 1) & (d <= me)
        tokens_left = left & (me == 1)
        tokens_right = right & (me == n - 2)

        @pl.when(tokens_left)
        def _():
            send(d, u, True, raw_rows).wait_recv()

        @pl.when(tokens_right)
        def _():
            send(d, u, False, raw_rows).wait_recv()

        @pl.when(tokens_left | tokens_right)
        def _():
            which = jnp.where(me == 1, 0, 1)
            more = arrived[which, d, u, :raw_rows, :].astype(F32)
            both = jnp.concatenate([level_tokens(d, u), more], 0).astype(BF)
            mine[d, u] = partial(both).astype(BF)

        @pl.when(jnp.logical_not(tokens_left | tokens_right))
        def _():
            mine[d, u] = partial(level_tokens(d, u).astype(BF)).astype(BF)

        @pl.when(left & (me > 1))
        def _():
            send(d, u, True, sum_rows).wait_recv()
            mine[d, u] = (mine[d, u].astype(F32) + arrived[0, d, u].astype(F32)).astype(BF)

        @pl.when(right & (me < n - 2))
        def _():
            send(d, u, False, sum_rows).wait_recv()
            mine[d, u] = (mine[d, u].astype(F32) + arrived[1, d, u].astype(F32)).astype(BF)

        @pl.when(d > me)
        def _():
            send(d, u, True, sum_rows).start()

        @pl.when(d < me)
        def _():
            send(d, u, False, sum_rows).start()

    def latent(u):
        total = mine[me, u].astype(F32)
        turned = jnp.concatenate([total[side:], jnp.zeros((8, width), F32)], 0).T.astype(BF)
        pooled = []
        query = []
        for a in range(latents):
            denom = dot(turned[a * LANES : (a + 1) * LANES], den_spread[...])[:tokens]
            pooled.append(total[a * tokens : (a + 1) * tokens] / denom)
            query.append(jnp.broadcast_to(lq[a : a + 1, :], (tokens, width)))
        pooled = jnp.concatenate(pooled, 0).astype(BF)
        value = (jnp.concatenate(query, 0) + dot(pooled, out_w[...])).astype(BF)
        i = lax.div(u, 2)

        @pl.when(lax.rem(u, 2) == 0)
        def _():
            head[i] = value
            send_head(i).start()

        @pl.when(lax.rem(u, 2) == 1)
        def _():
            tail[...] = value

    scale_row = jnp.zeros((1, LANES), F32)
    for h in range(heads):
        scale_row = jnp.where(iota((1, LANES), 1) == h, swin[h] / head_dim, scale_row)
    row = iota((2 * side, 2 * side), 0)
    col = iota((2 * side, 2 * side), 1)
    window = lax.rem(row, STEP) // WC == lax.rem(col, STEP) // WC
    region = (row >= side) == (col >= side)
    mask[...] = jnp.where(window & (region | (place < spaces - 1)), 1.0, 0.0)

    def layer(i):
        send_head(i).wait_recv()
        block = jnp.concatenate([tail[...].astype(F32), ahead[i].astype(F32)], 0)
        normed = layer_norm(block, attn_gain[...]).astype(BF)
        packed = dot(normed, qkv_w[...]).astype(BF)
        q = packed[:, :width]
        k = packed[:, width : 2 * width]
        v = packed[:, 2 * width :]
        q32 = q.astype(F32)
        k32 = k.astype(F32)
        q_norm = dot((q32 * q32).astype(BF), ones[...])
        q_norm = lax.rsqrt(q_norm * (1.0 / head_dim) + 1e-06) * scale_row
        k_norm = dot_t(ones_t[...], (k32 * k32).astype(BF))
        k_norm = lax.rsqrt(k_norm * (1.0 / head_dim) + 1e-06)
        mixed = []
        for h in range(heads):
            cut = slice(h * head_dim, (h + 1) * head_dim)
            scores = dot_t(q[:, cut], k[:, cut])
            scores = scores * q_norm[:, h : h + 1] * k_norm[h : h + 1, :]
            weights = jnp.exp(scores) * mask[...]
            norm = jnp.sum(weights, -1, keepdims=True)
            mixed.append(dot(weights.astype(BF), v[:, cut]) / norm)
        mixed = jnp.concatenate(mixed, 1).astype(BF)
        branch = dot(mixed, proj_w[...]).astype(BF)
        middle = block + branch.astype(F32)

        def feed(part):
            mlp_in = layer_norm(part, mlp_gain[...]).astype(BF)
            hidden = jax.nn.gelu(dot(mlp_in, up_w[...])).astype(BF)
            final = part + dot(hidden, down_w[...])
            return final.reshape(latents, SR, STEP, width).astype(BF)

        back[i] = feed(middle[side:])
        send_back(i).start()
        own[i] = feed(middle[:side])
        keep_own(i).start()

        @pl.when(i == 0)
        def _():
            for copy in edge_copies():
                copy.start()

    def step(v, carry):
        def body(k, c):
            d = dest_of(jnp.where(k == 0, 0, jnp.where(k == 1, n - 1, k - 1)))
            u = v - lead + lead_of(d)

            @pl.when((u >= 0) & (u < units) & ((d == me) | jnp.logical_not(is_end)))
            def _():
                collect(d, u)

            return c

        lax.fori_loop(0, n, body, 0)

        @pl.when(v == lead)
        def _():
            for copy in weights[3:]:
                copy.wait()

        @pl.when(v >= lead)
        def _():
            latent(v - lead)

            @pl.when(lax.rem(v - lead, 2) == 1)
            def _():
                layer(lax.div(v - lead, 2))

        return carry

    lax.fori_loop(0, units + lead, step, 0)

    def drain(d, u):
        @pl.when((d != me) & is_end)
        def _():
            send(d, u, True, raw_rows).wait_send()

        @pl.when((d != me) & jnp.logical_not(is_end))
        def _():
            send(d, u, True, sum_rows).wait_send()

    each_unit(0, total_steps, drain)

    def finish(i, carry):
        send_head(i).wait_send()
        keep_own(i).wait()
        send_back(i).wait()
        return carry

    lax.fori_loop(0, chunks, finish, 0)
    for copy in edge_copies():
        copy.wait()


def shards(
    levels_in,
    kv_gain,
    level_embed,
    latent_queries,
    q_weight,
    k_weight,
    v_weight,
    out_weight,
    perc_scale,
    attn_gain,
    qkv_weight,
    swin_scale,
    proj_weight,
    mlp_gain,
    up_weight,
    down_weight,
):
    levels, rows, all_cols, width = levels_in.shape
    latents = latent_queries.shape[0]
    heads = perc_scale.shape[0]
    mlp = up_weight.shape[1]
    n = lax.axis_size("level")
    cols = all_cols // n
    chunks = cols // STEP
    units = 2 * chunks
    tokens = SR * STEP
    side = latents * tokens
    sum_rows = side + 8
    assert rows == WR and heads == 8 and tokens <= LANES and latents * heads <= LANES
    assert cols % STEP == 0 and n >= 4 and levels * tokens <= sum_rows

    hbm = pl.BlockSpec(memory_space=pl.ANY)
    vmem = pl.BlockSpec(memory_space=pltpu.VMEM)
    smem = pl.BlockSpec(memory_space=pltpu.SMEM)
    sem = pltpu.SemaphoreType.DMA
    padded = pl.pallas_call(
        kernel,
        in_specs=[hbm, vmem, vmem, vmem, hbm, hbm, hbm, hbm, smem, vmem, hbm, smem, hbm, vmem]
        + [hbm, hbm],
        out_specs=hbm,
        out_shape=jax.ShapeDtypeStruct((latents, rows, cols + EDGE, width), BF),
        scratch_shapes=[
            pltpu.VMEM((width, width), BF),
            pltpu.VMEM((width, width), BF),
            pltpu.VMEM((width, width), BF),
            pltpu.VMEM((width, width), BF),
            pltpu.VMEM((width, 3 * width), BF),
            pltpu.VMEM((width, width), BF),
            pltpu.VMEM((width, mlp), BF),
            pltpu.VMEM((mlp, width), BF),
            pltpu.VMEM((n, units, levels, SR, STEP, width), BF),
            pltpu.VMEM((n, units, levels, SR, EDGE, width), BF),
            pltpu.VMEM((n, units, sum_rows, width), BF),
            pltpu.VMEM((2, n, units, sum_rows, width), BF),
            pltpu.VMEM((chunks, side, width), BF),
            pltpu.VMEM((side, width), BF),
            pltpu.VMEM((chunks, side, width), BF),
            pltpu.VMEM((chunks, latents, SR, STEP, width), BF),
            pltpu.VMEM((chunks, latents, SR, STEP, width), BF),
            pltpu.VMEM((2 * LANES, width), BF),
            pltpu.VMEM((width, LANES), BF),
            pltpu.VMEM((LANES, latents * width), BF),
            pltpu.VMEM((16, width), BF),
            pltpu.VMEM((16, width), BF),
            pltpu.VMEM((16, width), F32),
            pltpu.VMEM((2 * side, 2 * side), F32),
            sem((8,)),
            sem((n, units)),
            sem((n, units)),
            sem((n, units)),
            sem((2, n, units)),
            sem((chunks,)),
            sem((chunks,)),
            sem((chunks,)),
            sem((chunks,)),
            sem((chunks,)),
            sem((2,)),
            sem((2,)),
        ],
        compiler_params=pltpu.CompilerParams(
            collective_id=0, has_side_effects=True, vmem_limit_bytes=63 * 1024 * 1024
        ),
        name="whole",
    )(
        levels_in,
        kv_gain[None],
        level_embed,
        latent_queries,
        q_weight,
        k_weight,
        v_weight,
        out_weight,
        perc_scale,
        attn_gain[None],
        qkv_weight,
        swin_scale,
        proj_weight,
        mlp_gain[None],
        up_weight,
        down_weight,
    )
    return padded[:, :, EDGE - SC : EDGE - SC + cols]


def solution(mesh):
    placed = (P("level", "space", None, None), P(), P("level", None)) + (P(),) * 13
    return jax.shard_map(
        shards,
        mesh=mesh,
        in_specs=placed,
        out_specs=P(None, "space", "level", None),
        check_vma=False,
    )
```

```python
import functools

import jax
import jax.numpy as jnp
from jax import lax
from jax.experimental import pallas as pl
from jax.experimental.pallas import tpu as pltpu
from jax.sharding import PartitionSpec as P

WR = 6
WC = 12
SR = 3
SC = 6
LANES = 128
STEP = 2 * WC
EDGE = 8
LEAD = 3
BF = jnp.bfloat16
F32 = jnp.float32
MESH = pl.DeviceIdType.MESH


def dot(a, b):
    return jnp.dot(a, b, preferred_element_type=F32)


def dot_t(a, b):
    return lax.dot_general(a, b, (((1,), (1,)), ((), ())), preferred_element_type=F32)


def iota(shape, axis):
    return lax.broadcasted_iota(jnp.int32, shape, axis)


def layer_norm(values, gain):
    center = values - jnp.mean(values, -1, keepdims=True)
    spread = jnp.mean(center * center, -1, keepdims=True)
    return center * lax.rsqrt(spread + 1e-05) * gain


def kernel(
    levels_hbm,
    kv_gain,
    embed,
    lq,
    q_hbm,
    k_hbm,
    v_hbm,
    out_hbm,
    perc,
    attn_gain,
    qkv_hbm,
    swin,
    proj_hbm,
    mlp_gain,
    up_hbm,
    down_hbm,
    p_hbm,
    q_w,
    k_w,
    v_w,
    out_w,
    qkv_w,
    proj_w,
    up_w,
    down_w,
    xa,
    xb,
    mine,
    arrived,
    latent_rows,
    own,
    back,
    q_mat,
    ones,
    spread,
    den_spread,
    ones_t,
    padded,
    mask,
    middle,
    both,
    query,
    perm,
    perm_t,
    w_sem,
    xa_sem,
    xb_sem,
    x_send,
    z_send,
    z_recv,
    own_sem,
    back_send,
    back_recv,
    edge_send,
    edge_recv,
):
    levels, rows, all_cols, width = levels_hbm.shape
    latents = lq.shape[0]
    heads = perc.shape[0]
    head_dim = width // heads
    n = lax.axis_size("level")
    spaces = lax.axis_size("space")
    me = lax.axis_index("level")
    place = lax.axis_index("space")
    cols = all_cols // n
    chunks = cols // STEP
    units = 2 * chunks
    tokens = SR * STEP
    side = latents * tokens
    raw_rows = levels * tokens
    lead = LEAD
    win_rows = mask.shape[0]
    is_end = (me == 0) | (me == n - 1)

    up_level = lax.rem(me + 1, n)
    down_level = lax.rem(me + n - 1, n)
    up_space = lax.rem(place + 1, spaces)
    down_space = lax.rem(place + spaces - 1, spaces)

    barrier = pltpu.get_barrier_semaphore()
    for target in ({"space": up_space}, {"space": down_space}):
        pl.semaphore_signal(barrier, inc=1, device_id=target, device_id_type=MESH)

    @pl.when(me < n - 1)
    def _():
        pl.semaphore_signal(
            barrier, inc=1, device_id={"level": up_level}, device_id_type=MESH
        )

    @pl.when(me > 0)
    def _():
        pl.semaphore_signal(
            barrier, inc=1, device_id={"level": down_level}, device_id_type=MESH
        )

    def enter():
        pl.semaphore_wait(barrier, jnp.where(is_end, 3, 4))

    def dest_of(j):
        return jnp.where(2 * me < n, n - 1 - j, j)

    def lead_of(d):
        near = is_end & (jnp.abs(d - me) == 1)
        return jnp.where((d == me) | near, 0, jnp.where(d == dest_of(0), lead, lead - 1))

    def chunk_of(i):
        return lax.rem(i + chunks - 1, chunks)

    def weight_copies():
        pairs = (
            (q_hbm, q_w),
            (k_hbm, k_w),
            (v_hbm, v_w),
            (out_hbm, out_w),
            (qkv_hbm, qkv_w),
            (proj_hbm, proj_w),
            (up_hbm, up_w),
            (down_hbm, down_w),
        )
        return [pltpu.make_async_copy(a, b, w_sem.at[i]) for i, (a, b) in enumerate(pairs)]

    def chunk_and_side(u):
        order = u + jnp.where(u == 1, 1, jnp.where(u == 2, -1, 0))
        return lax.div(order, 2), lax.rem(order, 2)

    def x_spans(d, i):
        start = pl.multiple_of(d * cols + chunk_of(i) * STEP, EDGE)
        rest = pl.multiple_of(lax.rem(start + STEP, all_cols), EDGE)
        return pl.ds(start, STEP), pl.ds(rest, EDGE)

    def x_copies(d, u):
        main, more = x_spans(d, chunk_and_side(u)[0])
        band = pl.ds(SR, SR)
        return (
            pltpu.make_async_copy(levels_hbm.at[:, band, main], xa.at[d, u], xa_sem.at[d, u]),
            pltpu.make_async_copy(levels_hbm.at[:, band, more], xb.at[d, u], xb_sem.at[d, u]),
        )

    def x_sends(d, u):
        main, more = x_spans(d, chunk_and_side(u)[0])
        band = pl.ds(0, SR)
        return (
            pltpu.make_async_remote_copy(
                src_ref=levels_hbm.at[:, band, main],
                dst_ref=xa.at[d, u],
                send_sem=x_send.at[0],
                recv_sem=xa_sem.at[d, u],
                device_id={"space": down_space},
                device_id_type=MESH,
            ),
            pltpu.make_async_remote_copy(
                src_ref=levels_hbm.at[:, band, more],
                dst_ref=xb.at[d, u],
                send_sem=x_send.at[1],
                recv_sem=xb_sem.at[d, u],
                device_id={"space": down_space},
                device_id_type=MESH,
            ),
        )

    def each_unit(first, last, act):
        def body(k, carry):
            j = lax.rem(k, n)
            d = dest_of(jnp.where(j == 0, 0, jnp.where(j == 1, n - 2, jnp.where(j == n - 1, j, j - 1))))
            u = lax.div(k, n) - lead + lead_of(d)

            @pl.when((u >= 0) & (u < units))
            def _():
                act(d, u)

            return carry

        lax.fori_loop(first, last, body, 0)

    def start_x(d, u):
        @pl.when(chunk_and_side(u)[1] == 0)
        def _():
            for copy in x_copies(d, u):
                copy.start()

    def push_x(d, u):
        @pl.when(chunk_and_side(u)[1] == 1)
        def _():
            for copy in x_sends(d, u):
                copy.start()

    def send(d, u, right, count):
        return pltpu.make_async_remote_copy(
            src_ref=mine.at[d, u, pl.ds(0, count)],
            dst_ref=arrived.at[0 if right else 1, d, u, pl.ds(0, count)],
            send_sem=z_send.at[0],
            recv_sem=z_recv.at[0 if right else 1, d, u],
            device_id={"level": up_level if right else down_level},
            device_id_type=MESH,
        )

    sum_rows = mine.shape[2]

    def column_of(i):
        return pl.multiple_of(EDGE + chunk_of(i) * STEP, EDGE)

    def send_back(i):
        return pltpu.make_async_remote_copy(
            src_ref=back.at[i],
            dst_ref=p_hbm.at[:, pl.ds(0, SR), pl.ds(column_of(i), STEP)],
            send_sem=back_send.at[i],
            recv_sem=back_recv.at[i],
            device_id={"space": up_space},
            device_id_type=MESH,
        )

    def keep_own(i):
        return pltpu.make_async_copy(
            own.at[i],
            p_hbm.at[:, pl.ds(SR, SR), pl.ds(column_of(i), STEP)],
            own_sem.at[i],
        )

    def edge_copies():
        cut = pl.ds(STEP - EDGE, EDGE)
        return (
            pltpu.make_async_remote_copy(
                src_ref=own.at[0, :, :, cut],
                dst_ref=p_hbm.at[:, pl.ds(SR, SR), pl.ds(0, EDGE)],
                send_sem=edge_send.at[0],
                recv_sem=edge_recv.at[0],
                device_id={"level": up_level},
                device_id_type=MESH,
            ),
            pltpu.make_async_remote_copy(
                src_ref=back.at[0, :, :, cut],
                dst_ref=p_hbm.at[:, pl.ds(0, SR), pl.ds(0, EDGE)],
                send_sem=edge_send.at[1],
                recv_sem=edge_recv.at[1],
                device_id={"space": up_space, "level": up_level},
                device_id_type=MESH,
            ),
        )

    def level_tokens(d, u):
        @pl.when(chunk_and_side(u)[1] == 0)
        def _():
            for copy in x_copies(d, u):
                copy.wait()

        @pl.when(chunk_and_side(u)[1] == 1)
        def _():
            for copy in x_sends(d, u):
                copy.wait_recv()

        normed = []
        for l in range(levels):
            x = jnp.concatenate([xa[d, u, l].astype(F32), xb[d, u, l].astype(F32)], 1)
            x = x[:, SC : SC + STEP].reshape(tokens, width)
            normed.append(layer_norm(x, kv_gain[...]) + embed[l : l + 1, :])
        return jnp.concatenate(normed, 0)

    total_steps = (units + lead) * n
    early = (lead + 1) * n
    weights = weight_copies()
    each_unit(0, early, start_x)
    for copy in weights[:3]:
        copy.start()

    def send_tokens(d, u):
        @pl.when(d != me)
        def _():
            mine[d, u, :raw_rows, :] = level_tokens(d, u).astype(BF)

            @pl.when((d == dest_of(0)) & (u == 0))
            def _():
                enter()

            @pl.when(me == 0)
            def _():
                send(d, u, True, raw_rows).start()

            @pl.when(me == n - 1)
            def _():
                send(d, u, False, raw_rows).start()

    @pl.when(is_end)
    def _():
        each_unit(0, 1, send_tokens)

    @pl.when(jnp.logical_not(is_end))
    def _():
        enter()

    each_unit(0, total_steps, push_x)
    each_unit(early, total_steps, start_x)
    for copy in weights[3:]:
        copy.start()

    @pl.when(is_end)
    def _():
        each_unit(1, total_steps, send_tokens)

    ones[...] = (
        (iota((width, LANES), 0) // head_dim == lax.rem(iota((width, LANES), 1), heads))
        & (iota((width, LANES), 1) < latents * heads)
    ).astype(F32).astype(BF)
    for a in range(latents):
        spread[:, a * width : (a + 1) * width] = (
            iota((LANES, width), 0) == iota((LANES, width), 1) // head_dim + a * heads
        ).astype(F32).astype(BF)
    den_spread[...] = (iota((16, width), 0) == iota((16, width), 1) // head_dim).astype(F32).astype(BF)
    ones_t[...] = den_spread[...]

    padded[...] = jnp.zeros_like(padded)
    padded[0:latents, :] = lq[...]
    weights[0].wait()
    queries = dot(padded[...].astype(BF), q_w[...])[:8]
    squares = queries * queries
    lane8 = iota((8, width), 1) // head_dim
    factor = jnp.zeros((8, width), F32)
    for h in range(heads):
        mean = jnp.sum(jnp.where(lane8 == h, squares, 0.0), -1, keepdims=True) / head_dim
        scale = lax.rsqrt(mean + 1e-06) * (perc[h] / head_dim)
        factor = jnp.where(lane8 == h, scale, factor)
    unit = queries * factor
    own_head = iota((heads, width), 0) == iota((heads, width), 1) // head_dim
    parts = [jnp.where(own_head, unit[a : a + 1], 0.0) for a in range(latents)]
    parts.append(jnp.zeros((LANES - latents * heads, width), F32))
    q_rows = jnp.concatenate(parts, 0)
    q_high = q_rows.astype(BF)
    q_mat[:LANES, :] = q_high
    q_mat[LANES:, :] = (q_rows - q_high.astype(F32)).astype(BF)

    weights[1].wait()
    weights[2].wait()

    def partial(normed):
        keys = dot(normed, k_w[...]).astype(BF)
        values = dot(normed, v_w[...]).astype(BF).astype(F32)
        keys32 = keys.astype(F32)
        squares = dot((keys32 * keys32).astype(BF), ones[...])
        raw = dot_t(keys, q_mat[...])
        raw = raw[:, :LANES] + raw[:, LANES:]
        weights = jnp.exp(raw * lax.rsqrt(squares * (1.0 / head_dim) + 1e-06))
        denom = weights[:tokens]
        count = normed.shape[0] // tokens
        for l in range(1, count):
            denom = denom + weights[l * tokens : (l + 1) * tokens]
        low = weights.astype(BF)
        parts = []
        for a in range(latents):
            wide = dot(low, spread[:, a * width : (a + 1) * width]) * values
            numer = wide[:tokens]
            for l in range(1, count):
                numer = numer + wide[l * tokens : (l + 1) * tokens]
            parts.append(numer)
        turned = jnp.concatenate([denom, jnp.ones((LANES - tokens, LANES), F32)], 0).T
        row = [turned[a * 8 : a * 8 + 8, :] for a in range(latents)]
        row.append(jnp.ones((8, width - latents * LANES), F32))
        parts.append(jnp.concatenate(row, 1))
        return jnp.concatenate(parts, 0)

    def collect(d, u):
        left = (me > 0) & (d >= me)
        right = (me < n - 1) & (d <= me)
        tokens_left = left & (me == 1)
        tokens_right = right & (me == n - 2)

        both[:raw_rows, :] = level_tokens(d, u)

        @pl.when(tokens_left)
        def _():
            send(d, u, True, raw_rows).wait_recv()

        @pl.when(tokens_right)
        def _():
            send(d, u, False, raw_rows).wait_recv()

        @pl.when(tokens_left | tokens_right)
        def _():
            which = jnp.where(me == 1, 0, 1)
            both[raw_rows:, :] = arrived[which, d, u, :raw_rows, :].astype(F32)
            mine[d, u] = partial(both[...].astype(BF)).astype(BF)

        @pl.when(jnp.logical_not(tokens_left | tokens_right))
        def _():
            mine[d, u] = partial(both[:raw_rows, :].astype(BF)).astype(BF)

        @pl.when(left & (me > 1))
        def _():
            send(d, u, True, sum_rows).wait_recv()
            mine[d, u] = (mine[d, u].astype(F32) + arrived[0, d, u].astype(F32)).astype(BF)

        @pl.when(right & (me < n - 2))
        def _():
            send(d, u, False, sum_rows).wait_recv()
            mine[d, u] = (mine[d, u].astype(F32) + arrived[1, d, u].astype(F32)).astype(BF)

        @pl.when(d > me)
        def _():
            send(d, u, True, sum_rows).start()

        @pl.when(d < me)
        def _():
            send(d, u, False, sum_rows).start()

    def latent(u):
        total = mine[me, u].astype(F32)
        turned = jnp.concatenate([total[side:], jnp.zeros((8, width), F32)], 0).T.astype(BF)
        pooled = []
        for a in range(latents):
            denom = dot(turned[a * LANES : (a + 1) * LANES], den_spread[...])[:tokens]
            pooled.append(total[a * tokens : (a + 1) * tokens] / denom)
        pooled = jnp.concatenate(pooled, 0).astype(BF)
        pooled = dot(perm[...], pooled).astype(BF)
        i, which = chunk_and_side(u)
        latent_rows[lax.rem(i, 2), which] = (query[...] + dot(pooled, out_w[...])).astype(BF)

    scale_row = jnp.zeros((1, LANES), F32)
    for h in range(heads):
        scale_row = jnp.where(iota((1, LANES), 1) == h, swin[h] / head_dim, scale_row)
    part = win_rows // 2
    row = iota((win_rows, win_rows), 0)
    col = iota((win_rows, win_rows), 1)
    region = (row >= part) == (col >= part)
    valid = lax.rem(col, part) < side // 2
    mask[...] = jnp.where(valid & (region | (place < spaces - 1)), 1.0, 0.0)

    def place_of(spot):
        inner = lax.rem(spot, part)
        grid = lax.div(inner, WC) * STEP + lax.div(spot, part) * WC + lax.rem(inner, WC)
        return jnp.where(inner < side // 2, grid, -1)

    size = (win_rows, side)
    perm[...] = (place_of(iota(size, 0)) == iota(size, 1)).astype(F32).astype(BF)
    size = (side, win_rows)
    perm_t[...] = (place_of(iota(size, 1)) == iota(size, 0)).astype(F32).astype(BF)
    owner = lax.div(lax.rem(iota((win_rows, width), 0), part), SR * WC)
    rows_of = jnp.broadcast_to(lq[0:1, :], (win_rows, width))
    for a in range(1, latents):
        rows_of = jnp.where(owner == a, lq[a : a + 1, :], rows_of)
    query[...] = rows_of

    def attention(i):
        slot = lax.rem(i, 2)
        pieces = [
            latent_rows[slot, which, w * part : (w + 1) * part, :]
            for w in range(2)
            for which in range(2)
        ]
        block = jnp.concatenate(pieces, 0).astype(F32)
        normed = layer_norm(block, attn_gain[...]).astype(BF)
        packed = dot(normed, qkv_w[...]).astype(BF)
        q = packed[:, :width]
        k = packed[:, width : 2 * width]
        v = packed[:, 2 * width :]
        q32 = q.astype(F32)
        k32 = k.astype(F32)
        q_norm = dot((q32 * q32).astype(BF), ones[...])
        q_norm = lax.rsqrt(q_norm * (1.0 / head_dim) + 1e-06) * scale_row
        k_norm = dot_t(ones_t[...], (k32 * k32).astype(BF))
        k_norm = lax.rsqrt(k_norm * (1.0 / head_dim) + 1e-06)
        windows = []
        for w in range(2):
            here = slice(w * win_rows, (w + 1) * win_rows)
            mixed = []
            for h in range(heads):
                cut = slice(h * head_dim, (h + 1) * head_dim)
                scores = dot_t(q[here, cut], k[here, cut])
                scores = scores * q_norm[here, h : h + 1] * k_norm[h : h + 1, here]
                weights = jnp.exp(scores) * mask[...]
                norm = jnp.sum(weights, -1, keepdims=True)
                mixed.append(dot(weights.astype(BF), v[here, cut]) / norm)
            windows.append(jnp.concatenate(mixed, 1))
        mixed = jnp.concatenate(windows, 0).astype(BF)
        branch = dot(mixed, proj_w[...]).astype(BF)
        middle[slot] = block + branch.astype(F32)

    def feed(i, which):
        slot = lax.rem(i, 2)
        pieces = []
        for w in range(2):
            start = w * win_rows + which * part
            pieces.append(middle[slot, start : start + part, :])
        rows_in = jnp.concatenate(pieces, 0)
        mlp_in = layer_norm(rows_in, mlp_gain[...]).astype(BF)
        hidden = jax.nn.gelu(dot(mlp_in, up_w[...])).astype(BF)
        final = (rows_in + dot(hidden, down_w[...])).astype(BF)
        return dot(perm_t[...], final).reshape(latents, SR, STEP, width).astype(BF)

    def feed_back(i):
        back[i] = feed(i, 1)
        send_back(i).start()

    def feed_own(i):
        own[i] = feed(i, 0)
        keep_own(i).start()

        @pl.when(i == 0)
        def _():
            for copy in edge_copies():
                copy.start()

    def finish_unit(u):
        @pl.when(u == 0)
        def _():
            for copy in weights[3:]:
                copy.wait()

        @pl.when((u >= 0) & (u < units))
        def _():
            latent(u)

        even = lax.rem(u, 2) == 0

        @pl.when((u == 3) | ((u >= 4) & even))
        def _():
            feed_back(jnp.where(u == 3, 0, lax.div(u, 2) - 1))

        def feeds_own(k, c):
            feed_own(jnp.where(u == 3, 0, lax.div(u, 2) - 1 - k))
            return c

        one = (u == 3) | (even & (u >= 4) & (u != units - 2))
        count = jnp.where(u == units, 2, jnp.where(one, 1, 0))
        lax.fori_loop(0, count, feeds_own, 0)

        chunk, which = chunk_and_side(u)

        @pl.when((u >= 2) & (u < units) & (which == 1))
        def _():
            attention(chunk)

    def step(v, carry):
        def body(k, c):
            mine_at = jnp.where(2 * me < n, n - 1 - me, me)
            other = dest_of(jnp.where(k - 1 < mine_at, k - 1, k))
            d = jnp.where(k == 0, dest_of(0), jnp.where(k == 1, me, other))
            u = v - lead + lead_of(d)

            @pl.when((u >= 0) & (u < units) & ((d == me) | jnp.logical_not(is_end)))
            def _():
                collect(d, u)

            @pl.when(k == 1)
            def _():
                finish_unit(u)

            return c

        lax.fori_loop(0, n, body, 0)
        return carry

    lax.fori_loop(0, units + lead + 1, step, 0)

    def sent(count):
        return pltpu.make_async_remote_copy(
            src_ref=mine.at[pl.ds(0, n - 1), :, pl.ds(0, count)],
            dst_ref=arrived.at[0, pl.ds(0, n - 1), :, pl.ds(0, count)],
            send_sem=z_send.at[0],
            recv_sem=z_recv.at[0, 0, 0],
            device_id={"level": up_level},
            device_id_type=MESH,
        )

    @pl.when(is_end)
    def _():
        sent(raw_rows).wait_send()

    @pl.when(jnp.logical_not(is_end))
    def _():
        sent(sum_rows).wait_send()

    for which, (buffer, sem) in enumerate(((xa, xa_sem), (xb, xb_sem))):
        pushed = buffer.at[:, pl.ds(0, chunks)]
        pltpu.make_async_remote_copy(
            src_ref=pushed,
            dst_ref=pushed,
            send_sem=x_send.at[which],
            recv_sem=sem.at[0, 0],
            device_id={"space": down_space},
            device_id_type=MESH,
        ).wait_send()
    for i in range(chunks):
        keep_own(i).wait()
        send_back(i).wait()
    for copy in edge_copies():
        copy.wait()


def shards(
    levels_in,
    kv_gain,
    level_embed,
    latent_queries,
    q_weight,
    k_weight,
    v_weight,
    out_weight,
    perc_scale,
    attn_gain,
    qkv_weight,
    swin_scale,
    proj_weight,
    mlp_gain,
    up_weight,
    down_weight,
):
    levels, rows, all_cols, width = levels_in.shape
    latents = latent_queries.shape[0]
    heads = perc_scale.shape[0]
    mlp = up_weight.shape[1]
    n = lax.axis_size("level")
    cols = all_cols // n
    chunks = cols // STEP
    units = 2 * chunks
    tokens = SR * STEP
    side = latents * tokens
    sum_rows = side + 8
    win_rows = 2 * (-(-side // 32) * 16)
    assert rows == WR and heads == 8 and tokens <= LANES and latents * heads <= LANES
    assert cols % STEP == 0 and n >= 4 and chunks >= 4 and levels * tokens <= sum_rows

    hbm = pl.BlockSpec(memory_space=pl.ANY)
    vmem = pl.BlockSpec(memory_space=pltpu.VMEM)
    smem = pl.BlockSpec(memory_space=pltpu.SMEM)
    sem = pltpu.SemaphoreType.DMA
    padded = pl.pallas_call(
        kernel,
        in_specs=[hbm, vmem, vmem, vmem, hbm, hbm, hbm, hbm, smem, vmem, hbm, smem, hbm, vmem]
        + [hbm, hbm],
        out_specs=hbm,
        out_shape=jax.ShapeDtypeStruct((latents, rows, cols + EDGE, width), BF),
        scratch_shapes=[
            pltpu.VMEM((width, width), BF),
            pltpu.VMEM((width, width), BF),
            pltpu.VMEM((width, width), BF),
            pltpu.VMEM((width, width), BF),
            pltpu.VMEM((width, 3 * width), BF),
            pltpu.VMEM((width, width), BF),
            pltpu.VMEM((width, mlp), BF),
            pltpu.VMEM((mlp, width), BF),
            pltpu.VMEM((n, units, levels, SR, STEP, width), BF),
            pltpu.VMEM((n, units, levels, SR, EDGE, width), BF),
            pltpu.VMEM((n, units, sum_rows, width), BF),
            pltpu.VMEM((2, n, units, sum_rows, width), BF),
            pltpu.VMEM((2, 2, win_rows, width), BF),
            pltpu.VMEM((chunks, latents, SR, STEP, width), BF),
            pltpu.VMEM((chunks, latents, SR, STEP, width), BF),
            pltpu.VMEM((2 * LANES, width), BF),
            pltpu.VMEM((width, LANES), BF),
            pltpu.VMEM((LANES, latents * width), BF),
            pltpu.VMEM((16, width), BF),
            pltpu.VMEM((16, width), BF),
            pltpu.VMEM((16, width), F32),
            pltpu.VMEM((win_rows, win_rows), F32),
            pltpu.VMEM((2, 2 * win_rows, width), F32),
            pltpu.VMEM((2 * levels * tokens, width), F32),
            pltpu.VMEM((win_rows, width), F32),
            pltpu.VMEM((win_rows, side), BF),
            pltpu.VMEM((side, win_rows), BF),
            sem((8,)),
            sem((n, units)),
            sem((n, units)),
            sem((2,)),
            sem((1,)),
            sem((2, n, units)),
            sem((chunks,)),
            sem((chunks,)),
            sem((chunks,)),
            sem((2,)),
            sem((2,)),
        ],
        compiler_params=pltpu.CompilerParams(
            collective_id=0, has_side_effects=True, vmem_limit_bytes=63 * 1024 * 1024
        ),
        name="whole",
    )(
        levels_in,
        kv_gain[None],
        level_embed,
        latent_queries,
        q_weight,
        k_weight,
        v_weight,
        out_weight,
        perc_scale,
        attn_gain[None],
        qkv_weight,
        swin_scale,
        proj_weight,
        mlp_gain[None],
        up_weight,
        down_weight,
    )
    return padded[:, :, EDGE - SC : EDGE - SC + cols]


def solution(mesh):
    placed = (P("level", "space", None, None), P(), P("level", None)) + (P(),) * 13
    return jax.shard_map(
        shards,
        mesh=mesh,
        in_specs=placed,
        out_specs=P(None, "space", "level", None),
        check_vma=False,
    )
```

```python
import functools

import jax
import jax.numpy as jnp
from jax import lax
from jax.experimental import pallas as pl
from jax.experimental.pallas import tpu as pltpu
from jax.sharding import PartitionSpec as P

WR = 6
WC = 12
SR = 3
SC = 6
LANES = 128
STEP = 2 * WC
EDGE = 8
LEAD = 3
BF = jnp.bfloat16
F32 = jnp.float32
MESH = pl.DeviceIdType.MESH


def dot(a, b):
    return jnp.dot(a, b, preferred_element_type=F32)


def dot_t(a, b):
    return lax.dot_general(a, b, (((1,), (1,)), ((), ())), preferred_element_type=F32)


def iota(shape, axis):
    return lax.broadcasted_iota(jnp.int32, shape, axis)


def layer_norm(values, gain):
    center = values - jnp.mean(values, -1, keepdims=True)
    spread = jnp.mean(center * center, -1, keepdims=True)
    return center * lax.rsqrt(spread + 1e-05) * gain


def kernel(
    levels_hbm,
    kv_gain,
    embed,
    lq,
    q_hbm,
    k_hbm,
    v_hbm,
    out_hbm,
    perc,
    attn_gain,
    qkv_hbm,
    swin,
    proj_hbm,
    mlp_gain,
    up_hbm,
    down_hbm,
    p_hbm,
    q_w,
    k_w,
    v_w,
    out_w,
    qkv_w,
    proj_w,
    up_w,
    down_w,
    xa,
    xb,
    mine,
    arrived,
    latent_rows,
    own,
    back,
    q_mat,
    ones,
    spread,
    den_spread,
    ones_t,
    padded,
    mask,
    middle,
    both,
    query,
    perm,
    perm_t,
    w_sem,
    xa_sem,
    xb_sem,
    x_send,
    z_send,
    z_recv,
    own_sem,
    back_send,
    back_recv,
    edge_send,
    edge_recv,
):
    levels, rows, all_cols, width = levels_hbm.shape
    latents = lq.shape[0]
    heads = perc.shape[0]
    head_dim = width // heads
    n = lax.axis_size("level")
    spaces = lax.axis_size("space")
    me = lax.axis_index("level")
    place = lax.axis_index("space")
    cols = all_cols // n
    chunks = cols // STEP
    units = 2 * chunks
    tokens = SR * STEP
    side = latents * tokens
    raw_rows = levels * tokens
    lead = LEAD
    win_rows = mask.shape[0]
    is_end = (me == 0) | (me == n - 1)

    up_level = lax.rem(me + 1, n)
    down_level = lax.rem(me + n - 1, n)
    up_space = lax.rem(place + 1, spaces)
    down_space = lax.rem(place + spaces - 1, spaces)

    barrier = pltpu.get_barrier_semaphore()
    for target in ({"space": up_space}, {"space": down_space}):
        pl.semaphore_signal(barrier, inc=1, device_id=target, device_id_type=MESH)

    @pl.when(me < n - 1)
    def _():
        pl.semaphore_signal(
            barrier, inc=1, device_id={"level": up_level}, device_id_type=MESH
        )

    @pl.when(me > 0)
    def _():
        pl.semaphore_signal(
            barrier, inc=1, device_id={"level": down_level}, device_id_type=MESH
        )

    def enter():
        pl.semaphore_wait(barrier, jnp.where(is_end, 3, 4))

    def dest_of(j):
        return jnp.where(2 * me < n, n - 1 - j, j)

    def lead_of(d):
        near = is_end & (jnp.abs(d - me) == 1)
        return jnp.where((d == me) | near, 0, jnp.where(d == dest_of(0), lead, lead - 1))

    def chunk_of(i):
        return lax.rem(i + chunks - 1, chunks)

    def weight_copies():
        pairs = (
            (q_hbm, q_w),
            (k_hbm, k_w),
            (v_hbm, v_w),
            (out_hbm, out_w),
            (qkv_hbm, qkv_w),
            (proj_hbm, proj_w),
            (up_hbm, up_w),
            (down_hbm, down_w),
        )
        return [pltpu.make_async_copy(a, b, w_sem.at[i]) for i, (a, b) in enumerate(pairs)]

    def chunk_and_side(u):
        order = u + jnp.where(u == 1, 1, jnp.where(u == 2, -1, 0))
        return lax.div(order, 2), lax.rem(order, 2)

    def x_spans(d, i):
        start = pl.multiple_of(d * cols + chunk_of(i) * STEP, EDGE)
        rest = pl.multiple_of(lax.rem(start + STEP, all_cols), EDGE)
        return pl.ds(start, STEP), pl.ds(rest, EDGE)

    def x_copies(d, u):
        main, more = x_spans(d, chunk_and_side(u)[0])
        band = pl.ds(SR, SR)
        return (
            pltpu.make_async_copy(levels_hbm.at[:, band, main], xa.at[d, u], xa_sem.at[d, u]),
            pltpu.make_async_copy(levels_hbm.at[:, band, more], xb.at[d, u], xb_sem.at[d, u]),
        )

    def x_sends(d, u):
        main, more = x_spans(d, chunk_and_side(u)[0])
        band = pl.ds(0, SR)
        return (
            pltpu.make_async_remote_copy(
                src_ref=levels_hbm.at[:, band, main],
                dst_ref=xa.at[d, u],
                send_sem=x_send.at[0],
                recv_sem=xa_sem.at[d, u],
                device_id={"space": down_space},
                device_id_type=MESH,
            ),
            pltpu.make_async_remote_copy(
                src_ref=levels_hbm.at[:, band, more],
                dst_ref=xb.at[d, u],
                send_sem=x_send.at[1],
                recv_sem=xb_sem.at[d, u],
                device_id={"space": down_space},
                device_id_type=MESH,
            ),
        )

    def each_unit(first, last, act):
        def body(k, carry):
            j = lax.rem(k, n)
            d = dest_of(jnp.where(j == 0, 0, jnp.where(j == 1, n - 2, jnp.where(j == n - 1, j, j - 1))))
            u = lax.div(k, n) - lead + lead_of(d)

            @pl.when((u >= 0) & (u < units))
            def _():
                act(d, u)

            return carry

        lax.fori_loop(first, last, body, 0)

    def start_x(d, u):
        @pl.when(chunk_and_side(u)[1] == 0)
        def _():
            for copy in x_copies(d, u):
                copy.start()

    def push_x(d, u):
        @pl.when(chunk_and_side(u)[1] == 1)
        def _():
            for copy in x_sends(d, u):
                copy.start()

    def send(d, u, right, count):
        return pltpu.make_async_remote_copy(
            src_ref=mine.at[d, u, pl.ds(0, count)],
            dst_ref=arrived.at[0 if right else 1, d, u, pl.ds(0, count)],
            send_sem=z_send.at[0],
            recv_sem=z_recv.at[0 if right else 1, d, u],
            device_id={"level": up_level if right else down_level},
            device_id_type=MESH,
        )

    sum_rows = mine.shape[2]

    def column_of(i):
        return pl.multiple_of(EDGE + chunk_of(i) * STEP, EDGE)

    def send_back(i):
        return pltpu.make_async_remote_copy(
            src_ref=back.at[i],
            dst_ref=p_hbm.at[:, pl.ds(0, SR), pl.ds(column_of(i), STEP)],
            send_sem=back_send.at[i],
            recv_sem=back_recv.at[i],
            device_id={"space": up_space},
            device_id_type=MESH,
        )

    def keep_own(i):
        return pltpu.make_async_copy(
            own.at[i],
            p_hbm.at[:, pl.ds(SR, SR), pl.ds(column_of(i), STEP)],
            own_sem.at[i],
        )

    def edge_copies():
        cut = pl.ds(STEP - EDGE, EDGE)
        return (
            pltpu.make_async_remote_copy(
                src_ref=own.at[0, :, :, cut],
                dst_ref=p_hbm.at[:, pl.ds(SR, SR), pl.ds(0, EDGE)],
                send_sem=edge_send.at[0],
                recv_sem=edge_recv.at[0],
                device_id={"level": up_level},
                device_id_type=MESH,
            ),
            pltpu.make_async_remote_copy(
                src_ref=back.at[0, :, :, cut],
                dst_ref=p_hbm.at[:, pl.ds(0, SR), pl.ds(0, EDGE)],
                send_sem=edge_send.at[1],
                recv_sem=edge_recv.at[1],
                device_id={"space": up_space, "level": up_level},
                device_id_type=MESH,
            ),
        )

    def level_tokens(d, u):
        @pl.when(chunk_and_side(u)[1] == 0)
        def _():
            for copy in x_copies(d, u):
                copy.wait()

        @pl.when(chunk_and_side(u)[1] == 1)
        def _():
            for copy in x_sends(d, u):
                copy.wait_recv()

        normed = []
        for l in range(levels):
            x = jnp.concatenate([xa[d, u, l].astype(F32), xb[d, u, l].astype(F32)], 1)
            x = x[:, SC : SC + STEP].reshape(tokens, width)
            normed.append(layer_norm(x, kv_gain[...]) + embed[l : l + 1, :])
        return jnp.concatenate(normed, 0)

    total_steps = (units + lead) * n
    early = (lead + 1) * n
    weights = weight_copies()
    each_unit(0, early, start_x)
    for copy in weights[:3]:
        copy.start()

    def send_tokens(d, u):
        @pl.when(d != me)
        def _():
            mine[d, u, :raw_rows, :] = level_tokens(d, u).astype(BF)

            @pl.when((d == dest_of(0)) & (u == 0))
            def _():
                enter()

            @pl.when(me == 0)
            def _():
                send(d, u, True, raw_rows).start()

            @pl.when(me == n - 1)
            def _():
                send(d, u, False, raw_rows).start()

    @pl.when(is_end)
    def _():
        each_unit(0, 1, send_tokens)

    @pl.when(jnp.logical_not(is_end))
    def _():
        enter()

    each_unit(0, total_steps, push_x)
    each_unit(early, total_steps, start_x)
    for copy in weights[3:]:
        copy.start()

    @pl.when(is_end)
    def _():
        each_unit(1, total_steps, send_tokens)

    ones[...] = (
        (iota((width, LANES), 0) // head_dim == lax.rem(iota((width, LANES), 1), heads))
        & (iota((width, LANES), 1) < latents * heads)
    ).astype(F32).astype(BF)
    for a in range(latents):
        spread[:, a * width : (a + 1) * width] = (
            iota((LANES, width), 0) == iota((LANES, width), 1) // head_dim + a * heads
        ).astype(F32).astype(BF)
    den_spread[...] = (iota((16, width), 0) == iota((16, width), 1) // head_dim).astype(F32).astype(BF)
    ones_t[...] = den_spread[...]

    padded[...] = jnp.zeros_like(padded)
    padded[0:latents, :] = lq[...]
    weights[0].wait()
    queries = dot(padded[...].astype(BF), q_w[...])[:8]
    squares = queries * queries
    lane8 = iota((8, width), 1) // head_dim
    factor = jnp.zeros((8, width), F32)
    for h in range(heads):
        mean = jnp.sum(jnp.where(lane8 == h, squares, 0.0), -1, keepdims=True) / head_dim
        scale = lax.rsqrt(mean + 1e-06) * (perc[h] / head_dim)
        factor = jnp.where(lane8 == h, scale, factor)
    unit = queries * factor
    own_head = iota((heads, width), 0) == iota((heads, width), 1) // head_dim
    parts = [jnp.where(own_head, unit[a : a + 1], 0.0) for a in range(latents)]
    parts.append(jnp.zeros((LANES - latents * heads, width), F32))
    q_rows = jnp.concatenate(parts, 0)
    q_high = q_rows.astype(BF)
    q_mat[:LANES, :] = q_high
    q_mat[LANES:, :] = (q_rows - q_high.astype(F32)).astype(BF)

    weights[1].wait()
    weights[2].wait()

    def partial(normed):
        keys = dot(normed, k_w[...]).astype(BF)
        values = dot(normed, v_w[...]).astype(BF).astype(F32)
        keys32 = keys.astype(F32)
        squares = dot((keys32 * keys32).astype(BF), ones[...])
        raw = dot_t(keys, q_mat[...])
        raw = raw[:, :LANES] + raw[:, LANES:]
        weights = jnp.exp(raw * lax.rsqrt(squares * (1.0 / head_dim) + 1e-06))
        denom = weights[:tokens]
        count = normed.shape[0] // tokens
        for l in range(1, count):
            denom = denom + weights[l * tokens : (l + 1) * tokens]
        low = weights.astype(BF)
        parts = []
        for a in range(latents):
            wide = dot(low, spread[:, a * width : (a + 1) * width]) * values
            numer = wide[:tokens]
            for l in range(1, count):
                numer = numer + wide[l * tokens : (l + 1) * tokens]
            parts.append(numer)
        turned = jnp.concatenate([denom, jnp.ones((LANES - tokens, LANES), F32)], 0).T
        row = [turned[a * 8 : a * 8 + 8, :] for a in range(latents)]
        row.append(jnp.ones((8, width - latents * LANES), F32))
        parts.append(jnp.concatenate(row, 1))
        return jnp.concatenate(parts, 0)

    def collect(d, u):
        left = (me > 0) & (d >= me)
        right = (me < n - 1) & (d <= me)
        tokens_left = left & (me == 1)
        tokens_right = right & (me == n - 2)

        both[:raw_rows, :] = level_tokens(d, u)

        @pl.when(tokens_left)
        def _():
            send(d, u, True, raw_rows).wait_recv()

        @pl.when(tokens_right)
        def _():
            send(d, u, False, raw_rows).wait_recv()

        @pl.when(tokens_left | tokens_right)
        def _():
            which = jnp.where(me == 1, 0, 1)
            both[raw_rows:, :] = arrived[which, d, u, :raw_rows, :].astype(F32)
            mine[d, u] = partial(both[...].astype(BF)).astype(BF)

        @pl.when(jnp.logical_not(tokens_left | tokens_right))
        def _():
            mine[d, u] = partial(both[:raw_rows, :].astype(BF)).astype(BF)

        @pl.when(left & (me > 1))
        def _():
            send(d, u, True, sum_rows).wait_recv()
            mine[d, u] = (mine[d, u].astype(F32) + arrived[0, d, u].astype(F32)).astype(BF)

        @pl.when(right & (me < n - 2))
        def _():
            send(d, u, False, sum_rows).wait_recv()
            mine[d, u] = (mine[d, u].astype(F32) + arrived[1, d, u].astype(F32)).astype(BF)

        @pl.when(d > me)
        def _():
            send(d, u, True, sum_rows).start()

        @pl.when(d < me)
        def _():
            send(d, u, False, sum_rows).start()

    def latent(u):
        total = mine[me, u].astype(F32)
        turned = jnp.concatenate([total[side:], jnp.zeros((8, width), F32)], 0).T.astype(BF)
        pooled = []
        for a in range(latents):
            denom = dot(turned[a * LANES : (a + 1) * LANES], den_spread[...])[:tokens]
            pooled.append(total[a * tokens : (a + 1) * tokens] / denom)
        pooled = jnp.concatenate(pooled, 0).astype(BF)
        pooled = dot(perm[...], pooled).astype(BF)
        i, which = chunk_and_side(u)
        latent_rows[lax.rem(i, 2), which] = (query[...] + dot(pooled, out_w[...])).astype(BF)

    scale_row = jnp.zeros((1, LANES), F32)
    for h in range(heads):
        scale_row = jnp.where(iota((1, LANES), 1) == h, swin[h] / head_dim, scale_row)
    part = win_rows // 2
    row = iota((win_rows, win_rows), 0)
    col = iota((win_rows, win_rows), 1)
    region = (row >= part) == (col >= part)
    valid = lax.rem(col, part) < side // 2
    mask[...] = jnp.where(valid & (region | (place < spaces - 1)), 1.0, 0.0)

    def place_of(spot):
        inner = lax.rem(spot, part)
        grid = lax.div(inner, WC) * STEP + lax.div(spot, part) * WC + lax.rem(inner, WC)
        return jnp.where(inner < side // 2, grid, -1)

    size = (win_rows, side)
    perm[...] = (place_of(iota(size, 0)) == iota(size, 1)).astype(F32).astype(BF)
    size = (side, win_rows)
    perm_t[...] = (place_of(iota(size, 1)) == iota(size, 0)).astype(F32).astype(BF)
    owner = lax.div(lax.rem(iota((win_rows, width), 0), part), SR * WC)
    rows_of = jnp.broadcast_to(lq[0:1, :], (win_rows, width))
    for a in range(1, latents):
        rows_of = jnp.where(owner == a, lq[a : a + 1, :], rows_of)
    query[...] = rows_of

    def attention(i):
        slot = lax.rem(i, 2)
        pieces = [
            latent_rows[slot, which, w * part : (w + 1) * part, :]
            for w in range(2)
            for which in range(2)
        ]
        block = jnp.concatenate(pieces, 0).astype(F32)
        normed = layer_norm(block, attn_gain[...]).astype(BF)
        packed = dot(normed, qkv_w[...]).astype(BF)
        q = packed[:, :width]
        k = packed[:, width : 2 * width]
        v = packed[:, 2 * width :]
        q32 = q.astype(F32)
        k32 = k.astype(F32)
        q_norm = dot((q32 * q32).astype(BF), ones[...])
        q_norm = lax.rsqrt(q_norm * (1.0 / head_dim) + 1e-06) * scale_row
        k_norm = dot_t(ones_t[...], (k32 * k32).astype(BF))
        k_norm = lax.rsqrt(k_norm * (1.0 / head_dim) + 1e-06)
        windows = []
        for w in range(2):
            here = slice(w * win_rows, (w + 1) * win_rows)
            mixed = []
            for h in range(heads):
                cut = slice(h * head_dim, (h + 1) * head_dim)
                scores = dot_t(q[here, cut], k[here, cut])
                scores = scores * q_norm[here, h : h + 1] * k_norm[h : h + 1, here]
                weights = jnp.exp(scores) * mask[...]
                norm = jnp.sum(weights, -1, keepdims=True)
                mixed.append(dot(weights.astype(BF), v[here, cut]) / norm)
            windows.append(jnp.concatenate(mixed, 1))
        mixed = jnp.concatenate(windows, 0).astype(BF)
        branch = dot(mixed, proj_w[...]).astype(BF)
        middle[slot] = block + branch.astype(F32)

    def feed(i, which):
        slot = lax.rem(i, 2)
        pieces = []
        for w in range(2):
            start = w * win_rows + which * part
            pieces.append(middle[slot, start : start + part, :])
        rows_in = jnp.concatenate(pieces, 0)
        mlp_in = layer_norm(rows_in, mlp_gain[...]).astype(BF)
        hidden = jax.nn.gelu(dot(mlp_in, up_w[...])).astype(BF)
        final = (rows_in + dot(hidden, down_w[...])).astype(BF)
        return dot(perm_t[...], final).reshape(latents, SR, STEP, width).astype(BF)

    def feed_back(i):
        back[i] = feed(i, 1)
        send_back(i).start()

    def feed_own(i):
        own[i] = feed(i, 0)
        keep_own(i).start()

        @pl.when(i == 0)
        def _():
            for copy in edge_copies():
                copy.start()

    def finish_unit(u):
        @pl.when(u == 0)
        def _():
            for copy in weights[3:]:
                copy.wait()

        @pl.when((u >= 0) & (u < units))
        def _():
            latent(u)

        even = lax.rem(u, 2) == 0

        @pl.when((u == 3) | ((u >= 4) & even))
        def _():
            feed_back(jnp.where(u == 3, 0, lax.div(u, 2) - 1))

        def feeds_own(k, c):
            feed_own(jnp.where(u == 3, 0, lax.div(u, 2) - 1 - k))
            return c

        one = (u == 3) | (even & (u >= 4) & (u != units - 2))
        count = jnp.where(u == units, 2, jnp.where(one, 1, 0))
        lax.fori_loop(0, count, feeds_own, 0)

        chunk, which = chunk_and_side(u)

        @pl.when((u >= 2) & (u < units) & (which == 1))
        def _():
            attention(chunk)

    def step(v, carry):
        def body(k, c):
            mine_at = jnp.where(2 * me < n, n - 1 - me, me)
            other = dest_of(jnp.where(k - 1 < mine_at, k - 1, k))
            d = jnp.where(k == 0, dest_of(0), jnp.where(k == 1, me, other))
            u = v - lead + lead_of(d)

            @pl.when((u >= 0) & (u < units) & ((d == me) | jnp.logical_not(is_end)))
            def _():
                collect(d, u)

            @pl.when(k == 1)
            def _():
                finish_unit(u)

            return c

        lax.fori_loop(0, n, body, 0)
        return carry

    lax.fori_loop(0, units + lead + 1, step, 0)

    def sent(count):
        return pltpu.make_async_remote_copy(
            src_ref=mine.at[pl.ds(0, n - 1), :, pl.ds(0, count)],
            dst_ref=arrived.at[0, pl.ds(0, n - 1), :, pl.ds(0, count)],
            send_sem=z_send.at[0],
            recv_sem=z_recv.at[0, 0, 0],
            device_id={"level": up_level},
            device_id_type=MESH,
        )

    @pl.when(is_end)
    def _():
        sent(raw_rows).wait_send()

    @pl.when(jnp.logical_not(is_end))
    def _():
        sent(sum_rows).wait_send()

    for which, (buffer, sem) in enumerate(((xa, xa_sem), (xb, xb_sem))):
        pushed = buffer.at[:, pl.ds(0, chunks)]
        pltpu.make_async_remote_copy(
            src_ref=pushed,
            dst_ref=pushed,
            send_sem=x_send.at[which],
            recv_sem=sem.at[0, 0],
            device_id={"space": down_space},
            device_id_type=MESH,
        ).wait_send()
    for i in range(chunks):
        keep_own(i).wait()
        send_back(i).wait()
    for copy in edge_copies():
        copy.wait()


def shift_kernel(padded, out_hbm, ready, sems):
    latents, rows, cols, _ = ready.shape
    copies = []
    for a in range(latents):
        for r in range(rows):
            row = padded[a, r].astype(F32)
            ready[a, r] = row[EDGE - SC : EDGE - SC + cols].astype(BF)
        copy = pltpu.make_async_copy(ready.at[a], out_hbm.at[a], sems.at[a])
        copy.start()
        copies.append(copy)
    for copy in copies:
        copy.wait()


def shards(
    levels_in,
    kv_gain,
    level_embed,
    latent_queries,
    q_weight,
    k_weight,
    v_weight,
    out_weight,
    perc_scale,
    attn_gain,
    qkv_weight,
    swin_scale,
    proj_weight,
    mlp_gain,
    up_weight,
    down_weight,
):
    levels, rows, all_cols, width = levels_in.shape
    latents = latent_queries.shape[0]
    heads = perc_scale.shape[0]
    mlp = up_weight.shape[1]
    n = lax.axis_size("level")
    cols = all_cols // n
    chunks = cols // STEP
    units = 2 * chunks
    tokens = SR * STEP
    side = latents * tokens
    sum_rows = side + 8
    win_rows = 2 * (-(-side // 32) * 16)
    assert rows == WR and heads == 8 and tokens <= LANES and latents * heads <= LANES
    assert cols % STEP == 0 and n >= 4 and chunks >= 4 and levels * tokens <= sum_rows

    hbm = pl.BlockSpec(memory_space=pl.ANY)
    vmem = pl.BlockSpec(memory_space=pltpu.VMEM)
    smem = pl.BlockSpec(memory_space=pltpu.SMEM)
    sem = pltpu.SemaphoreType.DMA
    padded = pl.pallas_call(
        kernel,
        in_specs=[hbm, vmem, vmem, vmem, hbm, hbm, hbm, hbm, smem, vmem, hbm, smem, hbm, vmem]
        + [hbm, hbm],
        out_specs=vmem,
        out_shape=pltpu.VMEM((latents, rows, cols + EDGE, width), BF),
        scratch_shapes=[
            pltpu.VMEM((width, width), BF),
            pltpu.VMEM((width, width), BF),
            pltpu.VMEM((width, width), BF),
            pltpu.VMEM((width, width), BF),
            pltpu.VMEM((width, 3 * width), BF),
            pltpu.VMEM((width, width), BF),
            pltpu.VMEM((width, mlp), BF),
            pltpu.VMEM((mlp, width), BF),
            pltpu.VMEM((n, units, levels, SR, STEP, width), BF),
            pltpu.VMEM((n, units, levels, SR, EDGE, width), BF),
            pltpu.VMEM((n, units, sum_rows, width), BF),
            pltpu.VMEM((2, n, units, sum_rows, width), BF),
            pltpu.VMEM((2, 2, win_rows, width), BF),
            pltpu.VMEM((chunks, latents, SR, STEP, width), BF),
            pltpu.VMEM((chunks, latents, SR, STEP, width), BF),
            pltpu.VMEM((2 * LANES, width), BF),
            pltpu.VMEM((width, LANES), BF),
            pltpu.VMEM((LANES, latents * width), BF),
            pltpu.VMEM((16, width), BF),
            pltpu.VMEM((16, width), BF),
            pltpu.VMEM((16, width), F32),
            pltpu.VMEM((win_rows, win_rows), F32),
            pltpu.VMEM((2, 2 * win_rows, width), F32),
            pltpu.VMEM((2 * levels * tokens, width), F32),
            pltpu.VMEM((win_rows, width), F32),
            pltpu.VMEM((win_rows, side), BF),
            pltpu.VMEM((side, win_rows), BF),
            sem((8,)),
            sem((n, units)),
            sem((n, units)),
            sem((2,)),
            sem((1,)),
            sem((2, n, units)),
            sem((chunks,)),
            sem((chunks,)),
            sem((chunks,)),
            sem((2,)),
            sem((2,)),
        ],
        compiler_params=pltpu.CompilerParams(
            collective_id=0, has_side_effects=True, vmem_limit_bytes=59 * 1024 * 1024
        ),
        name="whole",
    )(
        levels_in,
        kv_gain[None],
        level_embed,
        latent_queries,
        q_weight,
        k_weight,
        v_weight,
        out_weight,
        perc_scale,
        attn_gain[None],
        qkv_weight,
        swin_scale,
        proj_weight,
        mlp_gain[None],
        up_weight,
        down_weight,
    )
    return pl.pallas_call(
        shift_kernel,
        in_specs=[vmem],
        out_specs=hbm,
        out_shape=jax.ShapeDtypeStruct((latents, rows, cols, width), BF),
        scratch_shapes=[pltpu.VMEM((latents, rows, cols, width), BF), sem((latents,))],
        compiler_params=pltpu.CompilerParams(vmem_limit_bytes=16 * 1024 * 1024),
        name="shift",
    )(padded)


def solution(mesh):
    placed = (P("level", "space", None, None), P(), P("level", None)) + (P(),) * 13
    return jax.shard_map(
        shards,
        mesh=mesh,
        in_specs=placed,
        out_specs=P(None, "space", "level", None),
        check_vma=False,
    )
```

```python
import functools

import jax
import jax.numpy as jnp
from jax import lax
from jax.experimental import pallas as pl
from jax.experimental.pallas import tpu as pltpu
from jax.sharding import PartitionSpec as P

WR = 6
WC = 12
SR = 3
SC = 6
LANES = 128
STEP = 2 * WC
EDGE = 8
LEAD = 3
BF = jnp.bfloat16
F32 = jnp.float32
MESH = pl.DeviceIdType.MESH


def dot(a, b):
    return jnp.dot(a, b, preferred_element_type=F32)


def dot_t(a, b):
    return lax.dot_general(a, b, (((1,), (1,)), ((), ())), preferred_element_type=F32)


def iota(shape, axis):
    return lax.broadcasted_iota(jnp.int32, shape, axis)


def layer_norm(values, gain):
    center = values - jnp.mean(values, -1, keepdims=True)
    spread = jnp.mean(center * center, -1, keepdims=True)
    return center * lax.rsqrt(spread + 1e-05) * gain


def kernel(
    levels_hbm,
    kv_gain,
    embed,
    lq,
    q_hbm,
    k_hbm,
    v_hbm,
    out_hbm,
    perc,
    attn_gain,
    qkv_hbm,
    swin,
    proj_hbm,
    mlp_gain,
    upadded_out,
    down_hbm,
    padded_out,
    q_w,
    k_w,
    v_w,
    out_w,
    qkv_w,
    proj_w,
    up_w,
    down_w,
    xa,
    xb,
    mine,
    arrived,
    latent_rows,
    own,
    back,
    q_mat,
    ones,
    spread,
    den_spread,
    ones_t,
    padded,
    mask,
    middle,
    both,
    query,
    perm,
    perm_t,
    w_sem,
    xa_sem,
    xb_sem,
    x_send,
    z_send,
    z_recv,
    back_send,
    back_recv,
    edge_send,
    edge_recv,
):
    levels, rows, all_cols, width = levels_hbm.shape
    latents = lq.shape[0]
    heads = perc.shape[0]
    head_dim = width // heads
    n = lax.axis_size("level")
    spaces = lax.axis_size("space")
    me = lax.axis_index("level")
    place = lax.axis_index("space")
    cols = all_cols // n
    chunks = cols // STEP
    units = 2 * chunks
    tokens = SR * STEP
    side = latents * tokens
    raw_rows = levels * tokens
    lead = LEAD
    win_rows = mask.shape[0]
    is_end = (me == 0) | (me == n - 1)

    up_level = lax.rem(me + 1, n)
    down_level = lax.rem(me + n - 1, n)
    up_space = lax.rem(place + 1, spaces)
    down_space = lax.rem(place + spaces - 1, spaces)

    barrier = pltpu.get_barrier_semaphore()
    pl.semaphore_signal(barrier, inc=1, device_id={"space": up_space}, device_id_type=MESH)

    @pl.when(me < n - 1)
    def _():
        pl.semaphore_signal(
            barrier, inc=1, device_id={"level": up_level}, device_id_type=MESH
        )

    @pl.when(me > 0)
    def _():
        pl.semaphore_signal(
            barrier, inc=1, device_id={"level": down_level}, device_id_type=MESH
        )

    def enter():
        pl.semaphore_wait(barrier, jnp.where(is_end, 2, 3))

    def dest_of(j):
        return jnp.where(2 * me < n, n - 1 - j, j)

    def lead_of(d):
        near = is_end & (jnp.abs(d - me) == 1)
        return jnp.where((d == me) | near, 0, jnp.where(d == dest_of(0), lead, lead - 1))

    def chunk_of(i):
        return lax.rem(i + chunks - 1, chunks)

    def weight_copies():
        pairs = (
            (q_hbm, q_w),
            (k_hbm, k_w),
            (v_hbm, v_w),
            (out_hbm, out_w),
            (qkv_hbm, qkv_w),
            (proj_hbm, proj_w),
            (upadded_out, up_w),
            (down_hbm, down_w),
        )
        return [pltpu.make_async_copy(a, b, w_sem.at[i]) for i, (a, b) in enumerate(pairs)]

    def chunk_and_side(u):
        order = u + jnp.where(u == 1, 1, jnp.where(u == 2, -1, 0))
        return lax.div(order, 2), lax.rem(order, 2)

    def x_spans(d, i):
        start = pl.multiple_of(d * cols + chunk_of(i) * STEP, EDGE)
        rest = pl.multiple_of(lax.rem(start + STEP, all_cols), EDGE)
        return pl.ds(start, STEP), pl.ds(rest, EDGE)

    def x_copies(d, u):
        main, more = x_spans(d, chunk_and_side(u)[0])
        band = pl.ds(SR, SR)
        return (
            pltpu.make_async_copy(levels_hbm.at[:, band, main], xa.at[d, u], xa_sem.at[d, u]),
            pltpu.make_async_copy(levels_hbm.at[:, band, more], xb.at[d, u], xb_sem.at[d, u]),
        )

    def x_sends(d, u):
        main, more = x_spans(d, chunk_and_side(u)[0])
        band = pl.ds(0, SR)
        return (
            pltpu.make_async_remote_copy(
                src_ref=levels_hbm.at[:, band, main],
                dst_ref=xa.at[d, u],
                send_sem=x_send.at[0],
                recv_sem=xa_sem.at[d, u],
                device_id={"space": down_space},
                device_id_type=MESH,
            ),
            pltpu.make_async_remote_copy(
                src_ref=levels_hbm.at[:, band, more],
                dst_ref=xb.at[d, u],
                send_sem=x_send.at[1],
                recv_sem=xb_sem.at[d, u],
                device_id={"space": down_space},
                device_id_type=MESH,
            ),
        )

    def each_unit(first, last, act):
        def body(k, carry):
            j = lax.rem(k, n)
            d = dest_of(jnp.where(j == 0, 0, jnp.where(j == 1, n - 2, jnp.where(j == n - 1, j, j - 1))))
            u = lax.div(k, n) - lead + lead_of(d)

            @pl.when((u >= 0) & (u < units))
            def _():
                act(d, u)

            return carry

        lax.fori_loop(first, last, body, 0)

    def start_x(d, u):
        @pl.when(chunk_and_side(u)[1] == 0)
        def _():
            for copy in x_copies(d, u):
                copy.start()

    def push_x(d, u):
        @pl.when(chunk_and_side(u)[1] == 1)
        def _():
            for copy in x_sends(d, u):
                copy.start()

    def send(d, u, right, count):
        return pltpu.make_async_remote_copy(
            src_ref=mine.at[d, u, pl.ds(0, count)],
            dst_ref=arrived.at[0 if right else 1, d, u, pl.ds(0, count)],
            send_sem=z_send.at[0],
            recv_sem=z_recv.at[0 if right else 1, d, u],
            device_id={"level": up_level if right else down_level},
            device_id_type=MESH,
        )

    sum_rows = mine.shape[2]

    def column_of(i):
        return pl.multiple_of(EDGE + chunk_of(i) * STEP, EDGE)

    def send_back(i):
        return pltpu.make_async_remote_copy(
            src_ref=back.at[i],
            dst_ref=padded_out.at[:, pl.ds(0, SR), pl.ds(column_of(i), STEP)],
            send_sem=back_send.at[i],
            recv_sem=back_recv.at[i],
            device_id={"space": up_space},
            device_id_type=MESH,
        )

    def edge_copies():
        cut = pl.ds(STEP - EDGE, EDGE)
        return (
            pltpu.make_async_remote_copy(
                src_ref=own,
                dst_ref=padded_out.at[:, pl.ds(SR, SR), pl.ds(0, EDGE)],
                send_sem=edge_send.at[0],
                recv_sem=edge_recv.at[0],
                device_id={"level": up_level},
                device_id_type=MESH,
            ),
            pltpu.make_async_remote_copy(
                src_ref=back.at[0, :, :, cut],
                dst_ref=padded_out.at[:, pl.ds(0, SR), pl.ds(0, EDGE)],
                send_sem=edge_send.at[1],
                recv_sem=edge_recv.at[1],
                device_id={"space": up_space, "level": up_level},
                device_id_type=MESH,
            ),
        )

    def level_tokens(d, u):
        @pl.when(chunk_and_side(u)[1] == 0)
        def _():
            for copy in x_copies(d, u):
                copy.wait()

        @pl.when(chunk_and_side(u)[1] == 1)
        def _():
            for copy in x_sends(d, u):
                copy.wait_recv()

        normed = []
        for l in range(levels):
            x = jnp.concatenate([xa[d, u, l].astype(F32), xb[d, u, l].astype(F32)], 1)
            x = x[:, SC : SC + STEP].reshape(tokens, width)
            normed.append(layer_norm(x, kv_gain[...]) + embed[l : l + 1, :])
        return jnp.concatenate(normed, 0)

    total_steps = (units + lead) * n
    weights = weight_copies()
    start_x(dest_of(0), 0)

    def send_tokens(d, u):
        @pl.when(d != me)
        def _():
            mine[d, u, :raw_rows, :] = level_tokens(d, u).astype(BF)

            @pl.when((d == dest_of(0)) & (u == 0))
            def _():
                enter()

            @pl.when(me == 0)
            def _():
                send(d, u, True, raw_rows).start()

            @pl.when(me == n - 1)
            def _():
                send(d, u, False, raw_rows).start()

    @pl.when(is_end)
    def _():
        each_unit(0, 1, send_tokens)

    @pl.when(jnp.logical_not(is_end))
    def _():
        enter()

    each_unit(1, total_steps, start_x)
    each_unit(1, total_steps, push_x)
    for copy in weights:
        copy.start()

    @pl.when(is_end)
    def _():
        each_unit(1, total_steps, send_tokens)

    ones[...] = (
        (iota((width, LANES), 0) // head_dim == lax.rem(iota((width, LANES), 1), heads))
        & (iota((width, LANES), 1) < latents * heads)
    ).astype(F32).astype(BF)
    for a in range(latents):
        spread[:, a * width : (a + 1) * width] = (
            iota((LANES, width), 0) == iota((LANES, width), 1) // head_dim + a * heads
        ).astype(F32).astype(BF)
    den_spread[...] = (iota((16, width), 0) == iota((16, width), 1) // head_dim).astype(F32).astype(BF)
    ones_t[...] = den_spread[...]

    padded[...] = jnp.zeros_like(padded)
    padded[0:latents, :] = lq[...]
    weights[0].wait()
    queries = dot(padded[...].astype(BF), q_w[...])[:8]
    squares = queries * queries
    lane8 = iota((8, width), 1) // head_dim
    factor = jnp.zeros((8, width), F32)
    for h in range(heads):
        mean = jnp.sum(jnp.where(lane8 == h, squares, 0.0), -1, keepdims=True) / head_dim
        scale = lax.rsqrt(mean + 1e-06) * (perc[h] / head_dim)
        factor = jnp.where(lane8 == h, scale, factor)
    unit = queries * factor
    own_head = iota((heads, width), 0) == iota((heads, width), 1) // head_dim
    parts = [jnp.where(own_head, unit[a : a + 1], 0.0) for a in range(latents)]
    parts.append(jnp.zeros((LANES - latents * heads, width), F32))
    q_rows = jnp.concatenate(parts, 0)
    q_high = q_rows.astype(BF)
    q_mat[:LANES, :] = q_high
    q_mat[LANES:, :] = (q_rows - q_high.astype(F32)).astype(BF)

    weights[1].wait()
    weights[2].wait()

    def partial(normed):
        keys = dot(normed, k_w[...]).astype(BF)
        values = dot(normed, v_w[...]).astype(BF).astype(F32)
        keys32 = keys.astype(F32)
        squares = dot((keys32 * keys32).astype(BF), ones[...])
        raw = dot_t(keys, q_mat[...])
        raw = raw[:, :LANES] + raw[:, LANES:]
        weights = jnp.exp(raw * lax.rsqrt(squares * (1.0 / head_dim) + 1e-06))
        denom = weights[:tokens]
        count = normed.shape[0] // tokens
        for l in range(1, count):
            denom = denom + weights[l * tokens : (l + 1) * tokens]
        low = weights.astype(BF)
        parts = []
        for a in range(latents):
            wide = dot(low, spread[:, a * width : (a + 1) * width]) * values
            numer = wide[:tokens]
            for l in range(1, count):
                numer = numer + wide[l * tokens : (l + 1) * tokens]
            parts.append(numer)
        turned = jnp.concatenate([denom, jnp.ones((LANES - tokens, LANES), F32)], 0).T
        row = [turned[a * 8 : a * 8 + 8, :] for a in range(latents)]
        row.append(jnp.ones((8, width - latents * LANES), F32))
        parts.append(jnp.concatenate(row, 1))
        return jnp.concatenate(parts, 0)

    def collect(d, u):
        left = (me > 0) & (d >= me)
        right = (me < n - 1) & (d <= me)
        tokens_left = left & (me == 1)
        tokens_right = right & (me == n - 2)

        both[:raw_rows, :] = level_tokens(d, u)

        @pl.when(tokens_left)
        def _():
            send(d, u, True, raw_rows).wait_recv()

        @pl.when(tokens_right)
        def _():
            send(d, u, False, raw_rows).wait_recv()

        @pl.when(tokens_left | tokens_right)
        def _():
            which = jnp.where(me == 1, 0, 1)
            both[raw_rows:, :] = arrived[which, d, u, :raw_rows, :].astype(F32)
            mine[d, u] = partial(both[...].astype(BF)).astype(BF)

        @pl.when(jnp.logical_not(tokens_left | tokens_right))
        def _():
            mine[d, u] = partial(both[:raw_rows, :].astype(BF)).astype(BF)

        @pl.when(left & (me > 1))
        def _():
            send(d, u, True, sum_rows).wait_recv()
            mine[d, u] = (mine[d, u].astype(F32) + arrived[0, d, u].astype(F32)).astype(BF)

        @pl.when(right & (me < n - 2))
        def _():
            send(d, u, False, sum_rows).wait_recv()
            mine[d, u] = (mine[d, u].astype(F32) + arrived[1, d, u].astype(F32)).astype(BF)

        @pl.when(d > me)
        def _():
            send(d, u, True, sum_rows).start()

        @pl.when(d < me)
        def _():
            send(d, u, False, sum_rows).start()

    def latent(u):
        total = mine[me, u].astype(F32)
        turned = jnp.concatenate([total[side:], jnp.zeros((8, width), F32)], 0).T.astype(BF)
        pooled = []
        for a in range(latents):
            denom = dot(turned[a * LANES : (a + 1) * LANES], den_spread[...])[:tokens]
            pooled.append(total[a * tokens : (a + 1) * tokens] / denom)
        pooled = jnp.concatenate(pooled, 0).astype(BF)
        pooled = dot(perm[...], pooled).astype(BF)
        i, which = chunk_and_side(u)
        latent_rows[lax.rem(i, 2), which] = (query[...] + dot(pooled, out_w[...])).astype(BF)

    scale_row = jnp.zeros((1, LANES), F32)
    for h in range(heads):
        scale_row = jnp.where(iota((1, LANES), 1) == h, swin[h] / head_dim, scale_row)
    part = win_rows // 2
    row = iota((win_rows, win_rows), 0)
    col = iota((win_rows, win_rows), 1)
    region = (row >= part) == (col >= part)
    valid = lax.rem(col, part) < side // 2
    mask[...] = jnp.where(valid & (region | (place < spaces - 1)), 1.0, 0.0)

    def place_of(spot):
        inner = lax.rem(spot, part)
        grid = lax.div(inner, WC) * STEP + lax.div(spot, part) * WC + lax.rem(inner, WC)
        return jnp.where(inner < side // 2, grid, -1)

    size = (win_rows, side)
    perm[...] = (place_of(iota(size, 0)) == iota(size, 1)).astype(F32).astype(BF)
    size = (side, win_rows)
    perm_t[...] = (place_of(iota(size, 1)) == iota(size, 0)).astype(F32).astype(BF)
    owner = lax.div(lax.rem(iota((win_rows, width), 0), part), SR * WC)
    rows_of = jnp.broadcast_to(lq[0:1, :], (win_rows, width))
    for a in range(1, latents):
        rows_of = jnp.where(owner == a, lq[a : a + 1, :], rows_of)
    query[...] = rows_of

    def attention(i):
        slot = lax.rem(i, 2)
        pieces = [
            latent_rows[slot, which, w * part : (w + 1) * part, :]
            for w in range(2)
            for which in range(2)
        ]
        block = jnp.concatenate(pieces, 0).astype(F32)
        normed = layer_norm(block, attn_gain[...]).astype(BF)
        packed = dot(normed, qkv_w[...]).astype(BF)
        q = packed[:, :width]
        k = packed[:, width : 2 * width]
        v = packed[:, 2 * width :]
        q32 = q.astype(F32)
        k32 = k.astype(F32)
        q_norm = dot((q32 * q32).astype(BF), ones[...])
        q_norm = lax.rsqrt(q_norm * (1.0 / head_dim) + 1e-06) * scale_row
        k_norm = dot_t(ones_t[...], (k32 * k32).astype(BF))
        k_norm = lax.rsqrt(k_norm * (1.0 / head_dim) + 1e-06)
        windows = []
        for w in range(2):
            here = slice(w * win_rows, (w + 1) * win_rows)
            mixed = []
            for h in range(heads):
                cut = slice(h * head_dim, (h + 1) * head_dim)
                scores = dot_t(q[here, cut], k[here, cut])
                scores = scores * q_norm[here, h : h + 1] * k_norm[h : h + 1, here]
                weights = jnp.exp(scores) * mask[...]
                norm = jnp.sum(weights, -1, keepdims=True)
                mixed.append(dot(weights.astype(BF), v[here, cut]) / norm)
            windows.append(jnp.concatenate(mixed, 1))
        mixed = jnp.concatenate(windows, 0).astype(BF)
        branch = dot(mixed, proj_w[...]).astype(BF)
        middle[slot] = block + branch.astype(F32)

    def feed(i, which):
        slot = lax.rem(i, 2)
        pieces = []
        for w in range(2):
            start = w * win_rows + which * part
            pieces.append(middle[slot, start : start + part, :])
        rows_in = jnp.concatenate(pieces, 0)
        mlp_in = layer_norm(rows_in, mlp_gain[...]).astype(BF)
        hidden = jax.nn.gelu(dot(mlp_in, up_w[...])).astype(BF)
        final = (rows_in + dot(hidden, down_w[...])).astype(BF)
        return dot(perm_t[...], final).reshape(latents, SR, STEP, width).astype(BF)

    def feed_back(i):
        back[i] = feed(i, 1)
        send_back(i).start()

    def feed_own(i):
        value = feed(i, 0)
        padded_out[:, SR:, pl.ds(column_of(i), STEP), :] = value

        @pl.when(i == 0)
        def _():
            own[...] = value[:, :, STEP - EDGE :]
            for copy in edge_copies():
                copy.start()

    def finish_unit(u):
        @pl.when(u == 0)
        def _():
            for copy in weights[3:]:
                copy.wait()

        @pl.when((u >= 0) & (u < units))
        def _():
            latent(u)

        even = lax.rem(u, 2) == 0

        @pl.when((u == 3) | ((u >= 4) & even))
        def _():
            feed_back(jnp.where(u == 3, 0, lax.div(u, 2) - 1))

        def feeds_own(k, c):
            feed_own(jnp.where(u == 3, 0, lax.div(u, 2) - 1 - k))
            return c

        one = (u == 3) | (even & (u >= 4) & (u != units - 2))
        count = jnp.where(u == units, 2, jnp.where(one, 1, 0))
        lax.fori_loop(0, count, feeds_own, 0)

        chunk, which = chunk_and_side(u)

        @pl.when((u >= 2) & (u < units) & (which == 1))
        def _():
            attention(chunk)

    def step(v, carry):
        def body(k, c):
            mine_at = jnp.where(2 * me < n, n - 1 - me, me)
            other = dest_of(jnp.where(k - 1 < mine_at, k - 1, k))
            d = jnp.where(k == 0, dest_of(0), jnp.where(k == 1, me, other))
            u = v - lead + lead_of(d)

            @pl.when((u >= 0) & (u < units) & ((d == me) | jnp.logical_not(is_end)))
            def _():
                collect(d, u)

            @pl.when(k == 1)
            def _():
                finish_unit(u)

            return c

        lax.fori_loop(0, n, body, 0)
        return carry

    lax.fori_loop(0, units + lead + 1, step, 0)

    def sent(count):
        return pltpu.make_async_remote_copy(
            src_ref=mine.at[pl.ds(0, n - 1), :, pl.ds(0, count)],
            dst_ref=arrived.at[0, pl.ds(0, n - 1), :, pl.ds(0, count)],
            send_sem=z_send.at[0],
            recv_sem=z_recv.at[0, 0, 0],
            device_id={"level": up_level},
            device_id_type=MESH,
        )

    @pl.when(is_end)
    def _():
        sent(raw_rows).wait_send()

    @pl.when(jnp.logical_not(is_end))
    def _():
        sent(sum_rows).wait_send()

    for which, (buffer, sem) in enumerate(((xa, xa_sem), (xb, xb_sem))):
        pushed = buffer.at[:, pl.ds(0, chunks)]
        pltpu.make_async_remote_copy(
            src_ref=pushed,
            dst_ref=pushed,
            send_sem=x_send.at[which],
            recv_sem=sem.at[0, 0],
            device_id={"space": down_space},
            device_id_type=MESH,
        ).wait_send()
    for i in range(chunks):
        send_back(i).wait()
    for copy in edge_copies():
        copy.wait()


def shift_kernel(padded, out_hbm, ready, sems):
    latents, rows, cols, _ = ready.shape
    copies = []
    for a in range(latents):
        for r in range(rows):
            row = padded[a, r].astype(F32)
            ready[a, r] = row[EDGE - SC : EDGE - SC + cols].astype(BF)
        copy = pltpu.make_async_copy(ready.at[a], out_hbm.at[a], sems.at[a])
        copy.start()
        copies.append(copy)
    for copy in copies:
        copy.wait()


def shards(
    levels_in,
    kv_gain,
    level_embed,
    latent_queries,
    q_weight,
    k_weight,
    v_weight,
    out_weight,
    perc_scale,
    attn_gain,
    qkv_weight,
    swin_scale,
    proj_weight,
    mlp_gain,
    up_weight,
    down_weight,
):
    levels, rows, all_cols, width = levels_in.shape
    latents = latent_queries.shape[0]
    heads = perc_scale.shape[0]
    mlp = up_weight.shape[1]
    n = lax.axis_size("level")
    cols = all_cols // n
    chunks = cols // STEP
    units = 2 * chunks
    tokens = SR * STEP
    side = latents * tokens
    sum_rows = side + 8
    win_rows = 2 * (-(-side // 32) * 16)
    assert rows == WR and heads == 8 and tokens <= LANES and latents * heads <= LANES
    assert cols % STEP == 0 and n >= 4 and chunks >= 4 and levels * tokens <= sum_rows

    hbm = pl.BlockSpec(memory_space=pl.ANY)
    vmem = pl.BlockSpec(memory_space=pltpu.VMEM)
    smem = pl.BlockSpec(memory_space=pltpu.SMEM)
    sem = pltpu.SemaphoreType.DMA
    padded = pl.pallas_call(
        kernel,
        in_specs=[hbm, vmem, vmem, vmem, hbm, hbm, hbm, hbm, smem, vmem, hbm, smem, hbm, vmem]
        + [hbm, hbm],
        out_specs=vmem,
        out_shape=pltpu.VMEM((latents, rows, cols + EDGE, width), BF),
        scratch_shapes=[
            pltpu.VMEM((width, width), BF),
            pltpu.VMEM((width, width), BF),
            pltpu.VMEM((width, width), BF),
            pltpu.VMEM((width, width), BF),
            pltpu.VMEM((width, 3 * width), BF),
            pltpu.VMEM((width, width), BF),
            pltpu.VMEM((width, mlp), BF),
            pltpu.VMEM((mlp, width), BF),
            pltpu.VMEM((n, units, levels, SR, STEP, width), BF),
            pltpu.VMEM((n, units, levels, SR, EDGE, width), BF),
            pltpu.VMEM((n, units, sum_rows, width), BF),
            pltpu.VMEM((2, n, units, sum_rows, width), BF),
            pltpu.VMEM((2, 2, win_rows, width), BF),
            pltpu.VMEM((latents, SR, EDGE, width), BF),
            pltpu.VMEM((chunks, latents, SR, STEP, width), BF),
            pltpu.VMEM((2 * LANES, width), BF),
            pltpu.VMEM((width, LANES), BF),
            pltpu.VMEM((LANES, latents * width), BF),
            pltpu.VMEM((16, width), BF),
            pltpu.VMEM((16, width), BF),
            pltpu.VMEM((16, width), F32),
            pltpu.VMEM((win_rows, win_rows), F32),
            pltpu.VMEM((2, 2 * win_rows, width), F32),
            pltpu.VMEM((2 * levels * tokens, width), F32),
            pltpu.VMEM((win_rows, width), F32),
            pltpu.VMEM((win_rows, side), BF),
            pltpu.VMEM((side, win_rows), BF),
            sem((8,)),
            sem((n, units)),
            sem((n, units)),
            sem((2,)),
            sem((1,)),
            sem((2, n, units)),
            sem((chunks,)),
            sem((chunks,)),
            sem((2,)),
            sem((2,)),
        ],
        compiler_params=pltpu.CompilerParams(
            collective_id=0, has_side_effects=True, vmem_limit_bytes=59 * 1024 * 1024
        ),
        name="whole",
    )(
        levels_in,
        kv_gain[None],
        level_embed,
        latent_queries,
        q_weight,
        k_weight,
        v_weight,
        out_weight,
        perc_scale,
        attn_gain[None],
        qkv_weight,
        swin_scale,
        proj_weight,
        mlp_gain[None],
        up_weight,
        down_weight,
    )
    return pl.pallas_call(
        shift_kernel,
        in_specs=[vmem],
        out_specs=hbm,
        out_shape=jax.ShapeDtypeStruct((latents, rows, cols, width), BF),
        scratch_shapes=[pltpu.VMEM((latents, rows, cols, width), BF), sem((latents,))],
        compiler_params=pltpu.CompilerParams(vmem_limit_bytes=16 * 1024 * 1024),
        name="shift",
    )(padded)


def solution(mesh):
    placed = (P("level", "space", None, None), P(), P("level", None)) + (P(),) * 13
    return jax.shard_map(
        shards,
        mesh=mesh,
        in_specs=placed,
        out_specs=P(None, "space", "level", None),
        check_vma=False,
    )
```
